128 devices in a mesh: row: 16 (over y, z), col: 8 (over x, core).
Axes of the slice: x: 4, y: 4, z: 4, core: 2. Of those that a mesh axis runs over, the one named last changes fastest.
Arguments:
- root_rhs: bfloat16 [8, 8192], replicated, may hold values from -6 to 6
- diag_inv: bfloat16 [16, 512, 512], replicated, may hold values from -1 to 2
- tile_u: bfloat16 [16, 8, 1, 2, 128, 512], P('row', 'col'), may hold values from -0.1875 to 0.1875
- tile_v: bfloat16 [16, 8, 1, 2, 512, 128], P('row', 'col'), may hold values from -0.25 to 0.25
- tile_rank: int32 [16, 8, 1, 2], P('row', 'col'), may hold values from 16 to 128
- child_x: bfloat16 [128, 8, 512], P(('row', 'col')), may hold values from -6 to 6
- border_t: bfloat16 [128, 512, 1024], P(('row', 'col')), may hold values from -0.09375 to 0.09375
- child_inv: bfloat16 [128, 512, 512], P(('row', 'col')), may hold values from -1 to 2
- child_blocks: int32 [128, 8], P(('row', 'col')), may hold values from 0 to 63
Outputs:
- root_solution: float32 [8, 8192], P(None, ('row', 'col'))
- child_out: float32 [128, 8, 512], P(('row', 'col'))
The draws below stay inside these ranges and needn't reach their ends.
All inputs are finite; a program needn't handle non-finite values.
Results may differ from the reference program's by a relative error of at most 0.017.
Values sent between devices are 32-bit elements; how exact they have to be, the bound alone decides.
A program may use at most 64 MiB of HBM per device.

```python
import math
import jax
import jax.numpy as jnp
import numpy as np
from jax import lax

NT = 16
TILE = 512
RHS = 8
RMAX = 128
BLK = 128
BB = 8
CSEP = 512
F = 8192
NB = 64
BORD = 1024
TR = 1
TC = 2
CHILDREN = 128
N_ROW = 16
N_COL = 8


def inverse_blocks(key, count, order):
    first, second_operand = jax.random.split(key, 2)
    diagonal = jax.random.uniform(first, (count, order), jnp.float32, 0.6, 1.2)
    spread = jnp.clip(jax.random.normal(second_operand, (count, order, order), jnp.float32), -6.0, 6.0)
    identity = jnp.eye(order, dtype=jnp.float32)
    blocks = spread * (0.5 / math.sqrt(order)) * (1.0 - identity) + identity[None] * diagonal[:, :, None]
    return blocks.astype(jnp.bfloat16)


def draw_diag_inv(key, part):
    return inverse_blocks(jax.random.fold_in(key, 11), NT, TILE)


def draw_child_inv(key, part):
    return inverse_blocks(jax.random.fold_in(key, 23), CHILDREN, CSEP)


def set_ends(entries, own_key, smallest, high):
    index_at = [jax.random.randint(jax.random.fold_in(own_key, axis), (), 0, length) for axis, length in enumerate(entries.shape)]
    longest = entries.shape.index(max(entries.shape))
    neighbour = index_at[:longest] + [(index_at[longest] + 1) % entries.shape[longest]] + index_at[longest + 1:]
    return entries.at[tuple(index_at)].set(smallest).at[tuple(neighbour)].set(high)


def block_scale(own_key, extent, cuts, least, high):
    def one(position, shards_of):
        steps = jax.random.uniform(jax.random.fold_in(jax.random.fold_in(own_key, 6), position), (shards_of,), jnp.float32, least / len(cuts), high / len(cuts))
        return jnp.repeat(jnp.exp(steps), extent[position] // shards_of).reshape((-1,) + (1,) * (len(extent) - position - 1))

    factor_of = one(*cuts[0])
    for cut in cuts[1:]:
        factor_of = factor_of * one(*cut)
    return factor_of


def rank_bounds(number_of, slope):
    weights = [(1 << 20) // math.isqrt(standing ** slope) + 1 for standing in range(1, number_of + 1)]
    scale = 1 + sum(weights) // (1 << 30)
    return np.cumsum(np.array([max(1, weight // scale) for weight in weights]))


def ranked(own_key, dims, amount, slope):
    table = rank_bounds(amount, slope)
    lot = jax.random.randint(jax.random.fold_in(own_key, 1), dims, 0, int(table[amount - 1]))
    standing = jnp.searchsorted(jnp.asarray(table, jnp.int32), lot, side="right")
    return jax.random.permutation(jax.random.fold_in(own_key, 2), amount)[standing].astype(jnp.int32)


def normal_values(stream_key, shape, scale, reach, cuts=(), kind=jnp.bfloat16):
    values = scale * jax.random.normal(stream_key, shape, jnp.float32)
    if cuts:
        values = values * block_scale(stream_key, shape, cuts, -0.22, 0.18)
    return jnp.clip(values, -reach, reach).astype(kind)


def setup_inputs(seed: int = 0) -> dict:
    splits = jax.random.split(jax.random.key(seed), 10)
    return {
        "root_rhs": normal_values(splits[0], (RHS, F), 1.0, 6.0),
        "diag_inv": draw_diag_inv(jax.random.fold_in(splits[9], 71), 0),
        "tile_u": normal_values(splits[2], (N_ROW, N_COL, TR, TC, RMAX, TILE), (RMAX * NT // 2) ** -0.5, 0.1875, ((0, 16), (1, 8))),
        "tile_v": normal_values(splits[3], (N_ROW, N_COL, TR, TC, TILE, RMAX), TILE ** -0.5, 0.25, ((0, 16), (1, 8))),
        "tile_rank": set_ends(jax.random.randint(splits[4], (N_ROW, N_COL, TR, TC), RMAX // 8, RMAX + 1), jax.random.fold_in(splits[4], 1), RMAX // 8, RMAX).astype(jnp.int32),
        "child_x": normal_values(splits[5], (CHILDREN, RHS, CSEP), 1.0, 6.0, ((0, 128),)),
        "border_t": normal_values(splits[6], (CHILDREN, CSEP, BORD), (CSEP * BB) ** -0.5, 0.09375, ((0, 128),)),
        "child_inv": draw_child_inv(jax.random.fold_in(splits[9], 71), 0),
        "child_blocks": set_ends(ranked(splits[8], (CHILDREN, BB), NB, 1), jax.random.fold_in(splits[8], 3), 0, NB - 1).astype(jnp.int32),
    }


def rounded_value(values):
    return lax.optimization_barrier(values.astype(jnp.bfloat16)).astype(jnp.float32)


def reference(root_rhs, diag_inv, tile_u, tile_v, tile_rank, child_x, border_t, child_inv, child_blocks):
    highest_precision = lax.Precision.HIGHEST
    upward = jnp.einsum('crs,csb->crb', child_x.astype(jnp.float32), border_t.astype(jnp.float32))
    pieces = upward.reshape(CHILDREN, RHS, BB, BLK).transpose(1, 0, 2, 3).reshape(RHS, CHILDREN * BB, BLK)
    flat_blocks = child_blocks.reshape(-1).astype(jnp.int32)
    dense_sum = jnp.zeros((RHS, NB, BLK), jnp.float32).at[:, flat_blocks, :].add(pieces)
    child_sum = dense_sum.reshape(RHS, NT, TILE)
    right_side = root_rhs.astype(jnp.float32).reshape(RHS, NT, TILE)
    inverses = diag_inv.astype(jnp.float32)
    rank_iota = jnp.arange(RMAX)
    tile_ids = jnp.arange(NT)
    solved_rows = jnp.zeros((RHS, NT, TILE), jnp.float32)
    for column in range(NT):
        owner_row, owner_slot = column % N_ROW, column // N_ROW
        left_rows = tile_u[owner_row, :, owner_slot].transpose(1, 0, 2, 3).reshape(NT, RMAX, TILE)
        right_row_indices = tile_v[owner_row, :, owner_slot].transpose(1, 0, 2, 3).reshape(NT, TILE, RMAX)
        rank_rows = tile_rank[owner_row, :, owner_slot].T.reshape(NT)
        live_mask = (rank_iota[None, :] < rank_rows[:, None]) & (tile_ids[:, None] < column)
        coefficient_values = jnp.einsum('gic,icw->giw', rounded_value(solved_rows), right_row_indices.astype(jnp.float32))
        coefficient_values = rounded_value(jnp.where(live_mask[None], coefficient_values, 0.0))
        partial_value = jnp.einsum('rkq,kqt->rt', coefficient_values, left_rows.astype(jnp.float32))
        row_total = partial_value + child_sum[:, column]
        fresh = jnp.dot(right_side[:, column] - row_total, inverses[column], precision=highest_precision)
        solved_rows = solved_rows.at[:, column].set(fresh)
    result = jnp.zeros((RHS, NT, TILE), jnp.float32)
    for column in reversed(range(NT)):
        owner_col, owner_slot = column % N_COL, column // N_COL
        left_cols = tile_u[:, owner_col, :, owner_slot].transpose(1, 0, 2, 3).reshape(NT, RMAX, TILE)
        right_cols = tile_v[:, owner_col, :, owner_slot].transpose(1, 0, 2, 3).reshape(NT, TILE, RMAX)
        rank_cols = tile_rank[:, owner_col, :, owner_slot].T.reshape(NT)
        live_mask = (rank_iota[None, :] < rank_cols[:, None]) & (tile_ids[:, None] > column)
        coefficient_values = jnp.einsum('rit,iqt->riq', rounded_value(result), left_cols.astype(jnp.float32))
        coefficient_values = rounded_value(jnp.where(live_mask[None], coefficient_values, 0.0))
        partial_value = jnp.einsum('riq,itq->rt', coefficient_values, right_cols.astype(jnp.float32))
        fresh = jnp.dot(solved_rows[:, column] - partial_value, inverses[column].T, precision=highest_precision)
        result = result.at[:, column].set(fresh)
    root_solution = result.reshape(RHS, F)
    gathered = result.reshape(RHS, NB, BLK)[:, flat_blocks, :].reshape(RHS, CHILDREN, BB * BLK)
    returned = jnp.einsum('rcb,csb->crs', rounded_value(gathered), border_t.astype(jnp.float32))
    child_out = child_x.astype(jnp.float32) - jnp.einsum('crs,cst->crt', returned, child_inv.astype(jnp.float32), precision=highest_precision)
    return root_solution, child_out
```

```python
import jax
import jax.numpy as jnp
from jax import lax
from jax.experimental import pallas as pl
from jax.experimental.pallas import tpu as pltpu
from jax.sharding import PartitionSpec as P

MESH = pl.DeviceIdType.MESH
F32 = jnp.float32
BF16 = jnp.bfloat16
NT = 16
TILE = 512
RHS = 8
RMAX = 128
BLK = 128
BB = 8
N_ROW = 16
N_COL = 8
G = 4
NG = NT // G
ZS = 0
HALF = TILE // N_COL
QB = TILE // BLK


def solver_col(group):
    return 3 + 2 * (group % 2)


def pair(i, j):
    return i * (i - 1) // 2 + j


def nn(a, b):
    return lax.dot_general(a, b, (((1,), (0,)), ((), ())), preferred_element_type=F32)


def nt(a, b):
    return lax.dot_general(a, b, (((1,), (1,)), ((), ())), preferred_element_type=F32)


def two_halves(t):
    hi = t.astype(BF16).astype(F32)
    return jnp.concatenate([hi, t - hi], axis=0).astype(BF16)


def folded(r):
    return r[:RHS] + r[RHS:]


def kernel(
    rhs_ref, cx_ref, blocks_ref, rank_ref, diag_hbm, u_hbm, v_hbm, bt_hbm, ci_hbm,
    root_out, child_out,
    bt_v, ci_v, u_v, v_v, d_v, us, vs, urx, vrx, ubf, vbf,
    childp, childrx, xrx, rowmsg, srx, xs, zfull, zs, bmsg, brx, tacc,
    lsem, csend, crecv, tsend, trecv, msend, srecv, xsend, xrecv,
    zsend, zrecv, bsend, brecv, gsend, grecv,
):
    row = lax.axis_index("row")
    col = lax.axis_index("col")
    a = row // G
    ii = row % G
    is_s = (ii == ZS) & (col == solver_col(a))
    srow = G * a + ZS
    scol = solver_col(a)
    ours = G * (a % 2)

    def remote(src, dst, send, recv, r, c):
        return pltpu.make_async_remote_copy(
            src_ref=src, dst_ref=dst, send_sem=send, recv_sem=recv,
            device_id=(r, c), device_id_type=MESH,
        )

    bar = pltpu.get_barrier_semaphore()

    def signal(r, c):
        pl.semaphore_signal(bar, inc=1, device_id=(r, c), device_id_type=MESH)

    @pl.loop(1, N_ROW)
    def _(k):
        signal((row + k) % N_ROW, col)

    for g in range(NG):
        @pl.when(jnp.logical_not((row == G * g + ZS) & (col == solver_col(g))))
        def _():
            signal(jnp.int32(G * g + ZS), jnp.int32(solver_col(g)))

    @pl.when(is_s)
    def _():
        me = row * N_COL + col

        @pl.loop(1, N_ROW * N_COL)
        def _(k):
            other = (me + k) % (N_ROW * N_COL)
            signal(other // N_COL, other % N_COL)

    loads = [
        pltpu.make_async_copy(bt_hbm.at[0], bt_v, lsem.at[0]),
        pltpu.make_async_copy(u_hbm.at[0, 0, 0], u_v, lsem.at[1]),
        pltpu.make_async_copy(v_hbm.at[0, 0, 0], v_v, lsem.at[2]),
        pltpu.make_async_copy(diag_hbm.at[pl.ds(G * a, G)], d_v, lsem.at[3]),
        pltpu.make_async_copy(ci_hbm.at[0], ci_v, lsem.at[4]),
    ]
    for load in loads:
        load.start()

    lane = lax.broadcasted_iota(jnp.int32, (RHS, RMAX), 1)
    live = [lane < rank_ref[0, 0, 0, b] for b in range(2)]

    loads[0].wait()
    up = nn(cx_ref[0], bt_v[...])
    pieces = [up[:, m * BLK:(m + 1) * BLK] for m in range(BB)]
    ids = [jnp.full((RHS, BLK), blocks_ref[0, m], jnp.int32) for m in range(BB)]

    @pl.loop(0, NT)
    def _(r):
        for q in range(QB):
            block = jnp.zeros((RHS, BLK), F32)
            for m in range(BB):
                block = block + jnp.where(ids[m] == r * (QB) + q, pieces[m], 0.0)
            childp[r, :, q * BLK:(q + 1) * BLK] = block

    loads[1].wait()
    loads[2].wait()
    slot = a // 2
    owner = (col // G == a % 2) & (col % G < ii)
    t_idx = ii * (ii - 1) // 2 + col % G

    @pl.when(owner)
    def _():
        us[...] = u_v[slot].astype(F32)
        wide = lax.broadcasted_iota(jnp.int32, (TILE, RMAX), 1)
        vs[...] = jnp.where(wide < rank_ref[0, 0, 0, slot], v_v[slot].astype(F32), 0.0)

    @pl.when(is_s)
    def _():
        pl.semaphore_wait(bar, N_ROW - 1 + NG - 1 + N_ROW * N_COL - 1)

    @pl.when(jnp.logical_not(is_s))
    def _():
        pl.semaphore_wait(bar, N_ROW - 1 + NG)

    def child_copy(k):
        peer = (row + k) % N_ROW
        return remote(childp.at[peer], childrx.at[k], csend.at[k], crecv.at[k], peer, col)

    @pl.loop(1, N_ROW)
    def _(k):
        child_copy(k).start()

    def tile_copies():
        return (
            remote(vs, vrx.at[t_idx], tsend.at[0], trecv.at[0, t_idx], srow, scol),
            remote(us, urx.at[t_idx], tsend.at[1], trecv.at[1, t_idx], srow, scol),
        )

    @pl.when(owner)
    def _():
        for copy in tile_copies():
            copy.start()

    @pl.loop(1, N_ROW)
    def _(k):
        child_copy(k).wait_recv()

    total = childp[row]
    for k in range(1, N_ROW):
        total = total + childrx[k]
    rowmsg[...] = total

    for b in range(2):
        @pl.when(col + N_COL * b < G * a)
        def _():
            remote(xs.at[0], xrx.at[b], xsend.at[0], xrecv.at[b], srow, scol).wait_recv()
            p = nn(xrx[b].astype(BF16), v_v[b])
            p = jnp.where(live[b], p, 0.0).astype(BF16)
            rowmsg[...] += nn(p, u_v[b])

    def row_copy():
        return remote(
            rowmsg, srx.at[ii, col], msend.at[0], srecv.at[ii, col], srow, scol
        )

    @pl.when(is_s)
    def _():
        srx[ZS, col] = rowmsg[...]

    @pl.when(jnp.logical_not(is_s))
    def _():
        row_copy().start()

    loads[3].wait()

    def x_copy(jj, da, i2):
        return remote(
            xs.at[jj], xrx.at[a // 2], xsend.at[(da * G + jj) * G + i2], xrecv.at[a // 2],
            G * (a + da) + i2, ours + jj,
        )

    @pl.when(is_s)
    def _():
        for t in range(G * (G - 1) // 2):
            remote(vs, vrx.at[t], tsend.at[0], trecv.at[0, t], srow, scol).wait_recv()
            remote(us, urx.at[t], tsend.at[1], trecv.at[1, t], srow, scol).wait_recv()
            vbf[t] = vrx[t].astype(BF16)
            ubf[t] = urx[t].astype(BF16)
        inner = [None] * G
        for jj in range(G):
            for c in range(N_COL):
                def wait_row():
                    remote(
                        rowmsg, srx.at[jj, c], msend.at[0], srecv.at[jj, c], srow, scol
                    ).wait_recv()

                if jj == ZS:
                    pl.when(col != c)(wait_row)
                else:
                    wait_row()
            tot = srx[jj, 0]
            for c in range(1, N_COL):
                tot = tot + srx[jj, c]
            if inner[jj] is not None:
                tot = tot + inner[jj]
            start = pl.multiple_of((G * a + jj) * TILE, TILE)
            right = rhs_ref[:, pl.ds(start, TILE)].astype(F32) - tot
            x = folded(nn(two_halves(right), d_v[jj]))
            xs[jj] = x

            @pl.when(a + 1 < NG)
            def _():
                for i2 in range(G):
                    x_copy(jj, 1, i2).start()

            xb = x.astype(BF16)
            for mm in range(jj + 1, G):
                t = pair(mm, jj)
                part = nn(nn(xb, vbf[t]).astype(BF16), ubf[t])
                inner[mm] = part if inner[mm] is None else inner[mm] + part
        for da in range(2, NG):
            @pl.when(a + da < NG)
            def _():
                for i2 in range(G):
                    for jj in range(G):
                        x_copy(jj, da, i2).start()

    def z_tile(i):
        return zfull.at[pl.ds(QB * i, QB)]

    def z_copy(jj, k):
        c = (G * ((a + 1) % 2) + k) % N_COL
        return c, remote(
            zs.at[jj], z_tile(G * a + jj), zsend.at[jj, k], zrecv.at[0], G * a + jj, c
        )

    @pl.when(is_s)
    def _():
        inner = [None] * G
        for jj in reversed(range(G)):
            tacc[...] = xs[jj]
            for da in reversed(range(1, NG)):
                @pl.when(a + da < NG)
                def _():
                    for i2 in range(G):
                        n = (da - 1) * G + i2
                        remote(
                            bmsg.at[0], brx.at[jj, n], bsend.at[0], brecv.at[jj, n], srow, scol
                        ).wait_recv()
                        tacc[...] -= brx[jj, n]
            left = tacc[...]
            if inner[jj] is not None:
                left = left - inner[jj]
            z = folded(nt(two_halves(left), d_v[jj]))
            for q in range(QB):
                zs[jj, q] = z[:, q * BLK:(q + 1) * BLK]
                if jj == ZS:
                    zfull[QB * row + q] = z[:, q * BLK:(q + 1) * BLK]
            for k in range(N_COL):
                c, copy = z_copy(jj, k)
                if jj == ZS:
                    pl.when(c != col)(copy.start)
                else:
                    copy.start()
            zb = z.astype(BF16)
            for mm in range(jj):
                t = pair(jj, mm)
                part = nt(nt(zb, ubf[t]).astype(BF16), vbf[t])
                inner[mm] = part if inner[mm] is None else inner[mm] + part

    @pl.when(jnp.logical_not(is_s))
    def _():
        remote(zs.at[0], z_tile(row), zsend.at[0, 0], zrecv.at[0], srow, scol).wait_recv()

    def back_copy(b):
        g = (col + N_COL * b) // G
        n = (a - g - 1) * G + ii
        return remote(
            bmsg.at[b], brx.at[col % G, n], bsend.at[b], brecv.at[col % G, n],
            G * g + ZS, solver_col(g),
        )

    mine = jnp.concatenate([zfull[QB * row + q] for q in range(QB)], axis=1)
    for b in reversed(range(2)):
        @pl.when(col + N_COL * b < G * a)
        def _():
            q = nt(mine.astype(BF16), u_v[b])
            q = jnp.where(live[b], q, 0.0).astype(BF16)
            bmsg[b] = nt(q, v_v[b])
            back_copy(b).start()

    def gather_copy(k):
        peer = (row + k) % N_ROW
        return remote(z_tile(row), z_tile(row), gsend.at[k], grecv.at[k], peer, col)

    @pl.loop(1, N_ROW)
    def _(k):
        gather_copy(k).start()

    wide = zfull[QB * row + col // 2]
    root_out[...] = jnp.where(col % 2 == 0, wide[:, :HALF], wide[:, HALF:])

    @pl.loop(1, N_ROW)
    def _(k):
        source = (row + N_ROW - k) % N_ROW
        remote(
            z_tile(source), z_tile(source), gsend.at[k], grecv.at[k], source, col
        ).wait_recv()

    loads[4].wait()
    parts = [zfull[blocks_ref[0, m]] for m in range(BB)]
    gathered = jnp.concatenate(parts, axis=1).astype(BF16)
    returned = nt(gathered, bt_v[...])
    child_out[0] = cx_ref[0].astype(F32) - folded(nn(two_halves(returned), ci_v[...]))

    @pl.loop(1, N_ROW)
    def _(k):
        child_copy(k).wait_send()
        gather_copy(k).wait_send()

    @pl.when(owner)
    def _():
        for copy in tile_copies():
            copy.wait_send()

    @pl.when(jnp.logical_not(is_s))
    def _():
        row_copy().wait_send()

    for b in range(2):
        @pl.when(col + N_COL * b < G * a)
        def _():
            back_copy(b).wait_send()

    @pl.when(is_s)
    def _():
        for da in range(1, NG):
            @pl.when(a + da < NG)
            def _():
                for i2 in range(G):
                    for jj in range(G):
                        x_copy(jj, da, i2).wait_send()
        for jj in range(G):
            for k in range(N_COL):
                c, copy = z_copy(jj, k)
                if jj == ZS:
                    pl.when(c != col)(copy.wait_send)
                else:
                    copy.wait_send()


def per_device(
    root_rhs, diag_inv, tile_u, tile_v, tile_rank, child_x, border_t, child_inv, child_blocks
):
    vmem = pl.BlockSpec(memory_space=pltpu.VMEM)
    smem = pl.BlockSpec(memory_space=pltpu.SMEM)
    hbm = pl.BlockSpec(memory_space=pl.ANY)
    dma = pltpu.SemaphoreType.DMA
    pairs = G * (G - 1) // 2
    wide = (RHS, TILE)
    return pl.pallas_call(
        kernel,
        out_shape=(
            jax.ShapeDtypeStruct((RHS, HALF), F32),
            jax.ShapeDtypeStruct((1, RHS, TILE), F32),
        ),
        in_specs=[vmem, vmem, smem, smem, hbm, hbm, hbm, hbm, hbm],
        out_specs=(vmem, vmem),
        scratch_shapes=[
            pltpu.VMEM((TILE, BB * BLK), BF16),
            pltpu.VMEM((TILE, TILE), BF16),
            pltpu.VMEM((2, RMAX, TILE), BF16),
            pltpu.VMEM((2, TILE, RMAX), BF16),
            pltpu.VMEM((G, TILE, TILE), BF16),
            pltpu.VMEM((RMAX, TILE), F32),
            pltpu.VMEM((TILE, RMAX), F32),
            pltpu.VMEM((pairs, RMAX, TILE), F32),
            pltpu.VMEM((pairs, TILE, RMAX), F32),
            pltpu.VMEM((pairs, RMAX, TILE), BF16),
            pltpu.VMEM((pairs, TILE, RMAX), BF16),
            pltpu.VMEM((NT, *wide), F32),
            pltpu.VMEM((N_ROW, *wide), F32),
            pltpu.VMEM((2, *wide), F32),
            pltpu.VMEM(wide, F32),
            pltpu.VMEM((G, N_COL, *wide), F32),
            pltpu.VMEM((G, *wide), F32),
            pltpu.VMEM((NT * QB, RHS, BLK), F32),
            pltpu.VMEM((G, QB, RHS, BLK), F32),
            pltpu.VMEM((2, *wide), F32),
            pltpu.VMEM((G, (NG - 1) * G, *wide), F32),
            pltpu.VMEM(wide, F32),
            dma((5,)),
            dma((N_ROW,)),
            dma((N_ROW,)),
            dma((2,)),
            dma((2, pairs)),
            dma((1,)),
            dma((G, N_COL)),
            dma((NG * G * G,)),
            dma((2,)),
            dma((G, N_COL)),
            dma((1,)),
            dma((2,)),
            dma((G, (NG - 1) * G)),
            dma((N_ROW,)),
            dma((N_ROW,)),
        ],
        compiler_params=pltpu.CompilerParams(
            collective_id=0, has_side_effects=True, vmem_limit_bytes=48 * 1024 * 1024
        ),
    )(
        root_rhs, child_x, child_blocks, tile_rank, diag_inv, tile_u, tile_v, border_t, child_inv
    )


def solution(mesh):
    both = ("row", "col")
    tiles = P("row", "col", None, None, None, None)
    in_specs = (
        P(),
        P(),
        tiles,
        tiles,
        P("row", "col", None, None),
        P(both, None, None),
        P(both, None, None),
        P(both, None, None),
        P(both, None),
    )
    out_specs = (P(None, both), P(both, None, None))
    return jax.shard_map(
        per_device, mesh=mesh, in_specs=in_specs, out_specs=out_specs, check_vma=False
    )
```

```python
import jax
import jax.numpy as jnp
from jax import lax
from jax.experimental import pallas as pl
from jax.experimental.pallas import tpu as pltpu
from jax.sharding import PartitionSpec as P

MESH = pl.DeviceIdType.MESH
F32 = jnp.float32
BF16 = jnp.bfloat16
NT = 16
TILE = 512
RHS = 8
RMAX = 128
BLK = 128
BB = 8
N_ROW = 16
N_COL = 8
G = 4
NG = NT // G
SOLVER_ROW = (3, 2, 0, 0)
SOLVER_COL = (3, 5, 5, 3)
HALF = TILE // N_COL
QB = TILE // BLK


def div(x, n):
    return lax.div(x, jnp.int32(n))


def mod(x, n):
    return lax.rem(x, jnp.int32(n))


def pick(table, group):
    if isinstance(group, int):
        return jnp.int32(table[group])
    value = jnp.int32(table[-1])
    for g in range(len(table) - 1):
        value = jnp.where(group == g, jnp.int32(table[g]), value)
    return value


def solver_of(group):
    return G * group + pick(SOLVER_ROW, group), pick(SOLVER_COL, group)


def pair(i, j):
    return i * (i - 1) // 2 + j


def nn(a, b):
    return lax.dot_general(a, b, (((1,), (0,)), ((), ())), preferred_element_type=F32)


def nt(a, b):
    return lax.dot_general(a, b, (((1,), (1,)), ((), ())), preferred_element_type=F32)


def two_halves(t):
    hi = t.astype(BF16).astype(F32)
    return jnp.concatenate([hi, t - hi], axis=0).astype(BF16)


def folded(r):
    return r[:RHS] + r[RHS:]


def kernel(
    rhs_hbm, cx_hbm, blocks_hbm, rank_hbm, diag_hbm, u_hbm, v_hbm, bt_hbm, ci_hbm,
    root_out, child_out,
    rhs_v, cx_v, blocks_s, rank_s,
    bt_v, ci_v, u_v, v_v, d_v, us, vs, urx, vrx, ubf, vbf,
    childp, childrx, xrx, rowmsg, srx, xs, zfull, zs, bmsg, brx, tacc,
    lsem, csend, crecv, tsend, trecv, msend, srecv, xsend, xrecv,
    zsend, zrecv, bsend, brecv, gsend, grecv,
):
    row = lax.axis_index("row")
    col = lax.axis_index("col")
    a = div(row, G)
    ii = mod(row, G)
    half = div(col, G)
    jcol = mod(col, G)
    srow, scol = solver_of(a)
    srel = srow - G * a
    is_s = (row == srow) & (col == scol)
    ours = G * mod(a, 2)

    width = G * TILE
    loads = [
        pltpu.make_async_copy(bt_hbm.at[0], bt_v, lsem.at[0]),
        pltpu.make_async_copy(cx_hbm.at[0], cx_v, lsem.at[1]),
        pltpu.make_async_copy(blocks_hbm, blocks_s, lsem.at[2]),
        pltpu.make_async_copy(rank_hbm.at[0, 0], rank_s, lsem.at[3]),
        pltpu.make_async_copy(u_hbm.at[0, 0, 0], u_v, lsem.at[4]),
        pltpu.make_async_copy(v_hbm.at[0, 0, 0], v_v, lsem.at[5]),
        pltpu.make_async_copy(
            rhs_hbm.at[:, pl.ds(pl.multiple_of(width * a, width), width)], rhs_v, lsem.at[6]
        ),
        pltpu.make_async_copy(diag_hbm.at[pl.ds(G * a, G)], d_v, lsem.at[7]),
        pltpu.make_async_copy(ci_hbm.at[0], ci_v, lsem.at[8]),
    ]
    for load in loads:
        load.start()

    def remote(src, dst, send, recv, r, c):
        return pltpu.make_async_remote_copy(
            src_ref=src, dst_ref=dst, send_sem=send, recv_sem=recv,
            device_id=(r, c), device_id_type=MESH,
        )

    bar = pltpu.get_barrier_semaphore()

    def signal(r, c):
        pl.semaphore_signal(bar, inc=1, device_id=(r, c), device_id_type=MESH)

    for k in range(1, N_ROW):
        signal(mod(row + k, N_ROW), col)

    @pl.when(jnp.logical_not(is_s))
    def _():
        signal(srow, scol)

    for b in range(2):
        @pl.when(half + 2 * b < a)
        def _():
            signal(*solver_of(half + 2 * b))

    @pl.when(is_s)
    def _():
        me = ii * N_COL + col
        for k in range(1, G * N_COL):
            other = mod(me + k, G * N_COL)
            signal(G * a + div(other, N_COL), mod(other, N_COL))
        for da in range(1, NG):
            @pl.when(a + da < NG)
            def _():
                for n in range(G * G):
                    signal(G * (a + da) + n // G, ours + n % G)

    greeted = (
        N_ROW - 1
        + jnp.where(is_s, G * N_COL - 1 + G * G * (NG - 1 - a), 1)
        + jnp.where(half < a, 1, 0)
        + jnp.where(half + 2 < a, 1, 0)
    )

    lane = lax.broadcasted_iota(jnp.int32, (RHS, RMAX), 1)
    loads[3].wait()
    live = [lane < rank_s[0, b] for b in range(2)]

    with jax.named_scope("up"):
        loads[1].wait()
        loads[2].wait()
        loads[0].wait()
        up = nn(cx_v[...], bt_v[...])
        pieces = [up[:, m * BLK:(m + 1) * BLK] for m in range(BB)]
        ids = [jnp.full((RHS, BLK), blocks_s[0, m], jnp.int32) for m in range(BB)]

        @pl.loop(0, NT)
        def _(r):
            for q in range(QB):
                block = jnp.zeros((RHS, BLK), F32)
                for m in range(BB):
                    block = block + jnp.where(ids[m] == r * (QB) + q, pieces[m], 0.0)
                childp[r, :, q * BLK:(q + 1) * BLK] = block

    loads[4].wait()
    loads[5].wait()
    slot = div(a, 2)
    owner = (half == mod(a, 2)) & (jcol < ii)
    t_idx = div(ii * (ii - 1), 2) + jcol
    own_tile = jnp.where(owner & is_s, t_idx, -1)

    @pl.when(owner)
    def _():
        us[...] = u_v[slot].astype(F32)
        wide = lax.broadcasted_iota(jnp.int32, (TILE, RMAX), 1)
        vs[...] = jnp.where(wide < rank_s[0, slot], v_v[slot].astype(F32), 0.0)

    @pl.when(owner & is_s)
    def _():
        urx[t_idx] = us[...]
        vrx[t_idx] = vs[...]

    with jax.named_scope("bar"):
        pl.semaphore_wait(bar, greeted)

    def child_copy(k):
        peer = mod(row + k, N_ROW)
        return remote(childp.at[peer], childrx.at[k], csend.at[k], crecv.at[k], peer, col)

    @pl.loop(1, N_ROW)
    def _(k):
        child_copy(k).start()

    def tile_copies():
        return (
            remote(vs, vrx.at[t_idx], tsend.at[0], trecv.at[0, t_idx], srow, scol),
            remote(us, urx.at[t_idx], tsend.at[1], trecv.at[1, t_idx], srow, scol),
        )

    @pl.when(owner & jnp.logical_not(is_s))
    def _():
        for copy in tile_copies():
            copy.start()

    with jax.named_scope("child_wait"):
        @pl.loop(1, N_ROW)
        def _(k):
            child_copy(k).wait_recv()

        total = childp[row]
        for k in range(1, N_ROW):
            total = total + childrx[k]
        rowmsg[...] = total

    with jax.named_scope("fwd_row"):
        for b in range(2):
            @pl.when(col + N_COL * b < G * a)
            def _():
                remote(xs.at[0], xrx.at[b], xsend.at[0], xrecv.at[b], srow, scol).wait_recv()
                p = nn(xrx[b].astype(BF16), v_v[b])
                p = jnp.where(live[b], p, 0.0).astype(BF16)
                rowmsg[...] += nn(p, u_v[b])

    def row_copy():
        return remote(
            rowmsg, srx.at[ii, col], msend.at[0], srecv.at[ii, col], srow, scol
        )

    @pl.when(is_s)
    def _():
        srx[ii, col] = rowmsg[...]

    @pl.when(jnp.logical_not(is_s))
    def _():
        row_copy().start()

    loads[6].wait()
    loads[7].wait()

    def x_copy(jj, da, i2):
        return remote(
            xs.at[jj], xrx.at[slot], xsend.at[(da * G + jj) * G + i2], xrecv.at[slot],
            G * (a + da) + i2, ours + jj,
        )

    @pl.when(is_s)
    def _():
        with jax.named_scope("tiles_wait"):
            for t in range(G * (G - 1) // 2):
                @pl.when(own_tile != t)
                def _():
                    remote(vs, vrx.at[t], tsend.at[0], trecv.at[0, t], srow, scol).wait_recv()
                    remote(us, urx.at[t], tsend.at[1], trecv.at[1, t], srow, scol).wait_recv()

                vbf[t] = vrx[t].astype(BF16)
                ubf[t] = urx[t].astype(BF16)
        inner = [None] * G
        for jj in range(G):
            with jax.named_scope(f"s_fwd_wait{jj}"):
                for c in range(N_COL):
                    def wait_row():
                        remote(
                            rowmsg, srx.at[jj, c], msend.at[0], srecv.at[jj, c], srow, scol
                        ).wait_recv()

                    pl.when((srel != jj) | (col != c))(wait_row)
            tot = srx[jj, 0]
            for c in range(1, N_COL):
                tot = tot + srx[jj, c]
            if inner[jj] is not None:
                tot = tot + inner[jj]
            right = rhs_v[:, jj * TILE:(jj + 1) * TILE].astype(F32) - tot
            x = folded(nn(two_halves(right), d_v[jj]))
            xs[jj] = x

            @pl.when(a + 1 < NG)
            def _():
                for i2 in range(G):
                    x_copy(jj, 1, i2).start()

            xb = x.astype(BF16)
            for mm in range(jj + 1, G):
                t = pair(mm, jj)
                part = nn(nn(xb, vbf[t]).astype(BF16), ubf[t])
                inner[mm] = part if inner[mm] is None else inner[mm] + part
        for da in range(2, NG):
            @pl.when(a + da < NG)
            def _():
                for i2 in range(G):
                    for jj in range(G):
                        x_copy(jj, da, i2).start()

    def z_tile(i):
        return zfull.at[pl.ds(QB * i, QB)]

    def z_copy(jj, k):
        c = mod(G - ours + k, N_COL)
        return c, remote(
            zs.at[jj], z_tile(G * a + jj), zsend.at[jj, k], zrecv.at[0], G * a + jj, c
        )

    @pl.when(is_s)
    def _():
        inner = [None] * G
        for jj in reversed(range(G)):
            with jax.named_scope(f"s_bwd_wait{jj}"):
                tacc[...] = xs[jj]
                for da in reversed(range(1, NG)):
                    @pl.when(a + da < NG)
                    def _():
                        for i2 in range(G):
                            n = (da - 1) * G + i2
                            remote(
                                bmsg.at[0], brx.at[jj, n], bsend.at[0], brecv.at[jj, n], srow, scol
                            ).wait_recv()
                            tacc[...] -= brx[jj, n]
            left = tacc[...]
            if inner[jj] is not None:
                left = left - inner[jj]
            z = folded(nt(two_halves(left), d_v[jj]))
            for q in range(QB):
                zs[jj, q] = z[:, q * BLK:(q + 1) * BLK]
                zfull[QB * (G * a + jj) + q] = z[:, q * BLK:(q + 1) * BLK]
            for k in range(N_COL):
                c, copy = z_copy(jj, k)
                pl.when((srel != jj) | (c != col))(copy.start)
            zb = z.astype(BF16)
            for mm in range(jj):
                t = pair(jj, mm)
                part = nt(nt(zb, ubf[t]).astype(BF16), vbf[t])
                inner[mm] = part if inner[mm] is None else inner[mm] + part

    @pl.when(jnp.logical_not(is_s))
    def _():
        with jax.named_scope("z_wait"):
            remote(zs.at[0], z_tile(row), zsend.at[0, 0], zrecv.at[0], srow, scol).wait_recv()

    def back_copy(b):
        g = half + 2 * b
        n = (a - g - 1) * G + ii
        return remote(
            bmsg.at[b], brx.at[jcol, n], bsend.at[b], brecv.at[jcol, n], *solver_of(g)
        )

    mine = jnp.concatenate([zfull[QB * row + q] for q in range(QB)], axis=1)
    for b in reversed(range(2)):
        @pl.when(col + N_COL * b < G * a)
        def _():
            q = nt(mine.astype(BF16), u_v[b])
            q = jnp.where(live[b], q, 0.0).astype(BF16)
            bmsg[b] = nt(q, v_v[b])
            back_copy(b).start()

    def gather_copy(k):
        peer = mod(row + k, N_ROW)
        return remote(z_tile(row), z_tile(row), gsend.at[k], grecv.at[k], peer, col)

    @pl.loop(1, N_ROW)
    def _(k):
        gather_copy(k).start()

    wide = zfull[QB * row + div(col, 2)]
    root_out[...] = jnp.where(mod(col, 2) == 0, wide[:, :HALF], wide[:, HALF:])

    with jax.named_scope("gather_wait"):
        @pl.loop(1, N_ROW)
        def _(k):
            source = mod(row + N_ROW - k, N_ROW)
            remote(
                z_tile(source), z_tile(source), gsend.at[k], grecv.at[k], source, col
            ).wait_recv()

    with jax.named_scope("final"):
        loads[8].wait()
        parts = [zfull[blocks_s[0, m]] for m in range(BB)]
        gathered = jnp.concatenate(parts, axis=1).astype(BF16)
        returned = nt(gathered, bt_v[...])
        child_out[0] = cx_v[...].astype(F32) - folded(nn(two_halves(returned), ci_v[...]))

    @pl.loop(1, N_ROW)
    def _(k):
        child_copy(k).wait_send()
        gather_copy(k).wait_send()

    @pl.when(owner & jnp.logical_not(is_s))
    def _():
        for copy in tile_copies():
            copy.wait_send()

    @pl.when(jnp.logical_not(is_s))
    def _():
        row_copy().wait_send()

    for b in range(2):
        @pl.when(col + N_COL * b < G * a)
        def _():
            back_copy(b).wait_send()

    @pl.when(is_s)
    def _():
        for da in range(1, NG):
            @pl.when(a + da < NG)
            def _():
                for i2 in range(G):
                    for jj in range(G):
                        x_copy(jj, da, i2).wait_send()
        for jj in range(G):
            for k in range(N_COL):
                c, copy = z_copy(jj, k)
                pl.when((srel != jj) | (c != col))(copy.wait_send)


def per_device(
    root_rhs, diag_inv, tile_u, tile_v, tile_rank, child_x, border_t, child_inv, child_blocks
):
    vmem = pl.BlockSpec(memory_space=pltpu.VMEM)
    hbm = pl.BlockSpec(memory_space=pltpu.HBM)
    dma = pltpu.SemaphoreType.DMA
    pairs = G * (G - 1) // 2
    wide = (RHS, TILE)
    return pl.pallas_call(
        kernel,
        out_shape=(
            jax.ShapeDtypeStruct((RHS, HALF), F32),
            jax.ShapeDtypeStruct((1, RHS, TILE), F32),
        ),
        in_specs=[hbm] * 9,
        out_specs=(vmem, vmem),
        scratch_shapes=[
            pltpu.VMEM((RHS, G * TILE), BF16),
            pltpu.VMEM(wide, BF16),
            pltpu.SMEM((1, BB), jnp.int32),
            pltpu.SMEM((1, 2), jnp.int32),
            pltpu.VMEM((TILE, BB * BLK), BF16),
            pltpu.VMEM((TILE, TILE), BF16),
            pltpu.VMEM((2, RMAX, TILE), BF16),
            pltpu.VMEM((2, TILE, RMAX), BF16),
            pltpu.VMEM((G, TILE, TILE), BF16),
            pltpu.VMEM((RMAX, TILE), F32),
            pltpu.VMEM((TILE, RMAX), F32),
            pltpu.VMEM((pairs, RMAX, TILE), F32),
            pltpu.VMEM((pairs, TILE, RMAX), F32),
            pltpu.VMEM((pairs, RMAX, TILE), BF16),
            pltpu.VMEM((pairs, TILE, RMAX), BF16),
            pltpu.VMEM((NT, *wide), F32),
            pltpu.VMEM((N_ROW, *wide), F32),
            pltpu.VMEM((2, *wide), F32),
            pltpu.VMEM(wide, F32),
            pltpu.VMEM((G, N_COL, *wide), F32),
            pltpu.VMEM((G, *wide), F32),
            pltpu.VMEM((NT * QB, RHS, BLK), F32),
            pltpu.VMEM((G, QB, RHS, BLK), F32),
            pltpu.VMEM((2, *wide), F32),
            pltpu.VMEM((G, (NG - 1) * G, *wide), F32),
            pltpu.VMEM(wide, F32),
            dma((9,)),
            dma((N_ROW,)),
            dma((N_ROW,)),
            dma((2,)),
            dma((2, pairs)),
            dma((1,)),
            dma((G, N_COL)),
            dma((NG * G * G,)),
            dma((2,)),
            dma((G, N_COL)),
            dma((1,)),
            dma((2,)),
            dma((G, (NG - 1) * G)),
            dma((N_ROW,)),
            dma((N_ROW,)),
        ],
        compiler_params=pltpu.CompilerParams(
            collective_id=0, has_side_effects=True, vmem_limit_bytes=67_043_328
        ),
    )(
        root_rhs, child_x, child_blocks, tile_rank, diag_inv, tile_u, tile_v, border_t, child_inv
    )


def solution(mesh):
    both = ("row", "col")
    tiles = P("row", "col", None, None, None, None)
    in_specs = (
        P(),
        P(),
        tiles,
        tiles,
        P("row", "col", None, None),
        P(both, None, None),
        P(both, None, None),
        P(both, None, None),
        P(both, None),
    )
    out_specs = (P(None, both), P(both, None, None))
    return jax.shard_map(
        per_device, mesh=mesh, in_specs=in_specs, out_specs=out_specs, check_vma=False
    )
```

```python
import jax
import jax.numpy as jnp
from jax import lax
from jax.experimental import pallas as pl
from jax.experimental.pallas import tpu as pltpu
from jax.sharding import PartitionSpec as P

MESH = pl.DeviceIdType.MESH
F32 = jnp.float32
BF16 = jnp.bfloat16
NT = 16
TILE = 512
RHS = 8
RMAX = 128
BLK = 128
BB = 8
N_ROW = 16
N_COL = 8
G = 4
NG = NT // G
SOLVER_ROW = (3, 3, 2, 0)
SOLVER_COL = (1, 5, 7, 3)
SOURCE = (2, 0)
RELAY = (3, 3)
HALF = TILE // N_COL
QB = TILE // BLK


def div(x, n):
    return lax.div(x, jnp.int32(n))


def mod(x, n):
    return lax.rem(x, jnp.int32(n))


def pick(table, group):
    if isinstance(group, int):
        return jnp.int32(table[group])
    value = jnp.int32(table[-1])
    for g in range(len(table) - 1):
        value = jnp.where(group == g, jnp.int32(table[g]), value)
    return value


def solver_of(group):
    return G * group + pick(SOLVER_ROW, group), pick(SOLVER_COL, group)


def pair(i, j):
    return i * (i - 1) // 2 + j


def nn(a, b):
    return lax.dot_general(a, b, (((1,), (0,)), ((), ())), preferred_element_type=F32)


def nt(a, b):
    return lax.dot_general(a, b, (((1,), (1,)), ((), ())), preferred_element_type=F32)


def two_halves(t):
    hi = t.astype(BF16).astype(F32)
    return jnp.concatenate([hi, t - hi], axis=0).astype(BF16)


def folded(r):
    return r[:RHS] + r[RHS:]


def kernel(
    rhs_hbm, cx_hbm, blocks_hbm, rank_hbm, diag_hbm, u_hbm, v_hbm, bt_hbm, ci_hbm,
    root_out, child_out,
    rhs_v, cx_v, blocks_s, rank_s, urelay, dt, ut, vt, utin, vtin,
    bt_v, ci_v, u_v, v_v, d_v, us, vs, urx, vrx, ubf, vbf,
    childp, childrx, xrx, rowmsg, srx, xs, zfull, zs, bmsg, brx, tacc,
    lsem, csend, crecv, tsend, trecv, msend, srecv, xsend, xrecv,
    zsend, zrecv, bsend, brecv, gsend, grecv, rsend, rrecv,
):
    row = lax.axis_index("row")
    col = lax.axis_index("col")
    a = div(row, G)
    ii = mod(row, G)
    half = div(col, G)
    jcol = mod(col, G)
    srow, scol = solver_of(a)
    srel = srow - G * a
    is_s = (row == srow) & (col == scol)
    ours = G * mod(a, 2)
    is_source = (row == SOURCE[0]) & (col == SOURCE[1])
    is_relay = (row == RELAY[0]) & (col == RELAY[1])

    width = G * TILE
    loads = [
        pltpu.make_async_copy(bt_hbm.at[0], bt_v, lsem.at[0]),
        pltpu.make_async_copy(cx_hbm.at[0], cx_v, lsem.at[1]),
        pltpu.make_async_copy(blocks_hbm, blocks_s, lsem.at[2]),
        pltpu.make_async_copy(rank_hbm.at[0, 0], rank_s, lsem.at[3]),
        pltpu.make_async_copy(u_hbm.at[0, 0, 0], u_v, lsem.at[4]),
        pltpu.make_async_copy(v_hbm.at[0, 0, 0], v_v, lsem.at[5]),
        pltpu.make_async_copy(
            rhs_hbm.at[:, pl.ds(pl.multiple_of(width * a, width), width)], rhs_v, lsem.at[6]
        ),
        pltpu.make_async_copy(diag_hbm.at[pl.ds(G * a, G)], d_v, lsem.at[7]),
        pltpu.make_async_copy(ci_hbm.at[0], ci_v, lsem.at[8]),
    ]
    for load in loads:
        load.start()

    def remote(src, dst, send, recv, r, c):
        return pltpu.make_async_remote_copy(
            src_ref=src, dst_ref=dst, send_sem=send, recv_sem=recv,
            device_id=(r, c), device_id_type=MESH,
        )

    bar = pltpu.get_barrier_semaphore()

    def signal(r, c):
        pl.semaphore_signal(bar, inc=1, device_id=(r, c), device_id_type=MESH)

    for k in range(1, N_ROW):
        signal(mod(row + k, N_ROW), col)

    @pl.when(jnp.logical_not(is_s))
    def _():
        signal(srow, scol)

    for b in range(2):
        @pl.when(half + 2 * b < a)
        def _():
            signal(*solver_of(half + 2 * b))

    @pl.when(is_s)
    def _():
        me = ii * N_COL + col
        for k in range(1, G * N_COL):
            other = mod(me + k, G * N_COL)
            signal(G * a + div(other, N_COL), mod(other, N_COL))
        for da in range(1, NG):
            @pl.when(a + da < NG)
            def _():
                for n in range(G * G):
                    signal(G * (a + da) + n // G, ours + n % G)

    @pl.when(is_source)
    def _():
        signal(jnp.int32(RELAY[0]), jnp.int32(RELAY[1]))

    @pl.when(is_relay)
    def _():
        signal(jnp.int32(SOURCE[0]), jnp.int32(SOURCE[1]))

    greeted = (
        N_ROW - 1
        + jnp.where(is_source | is_relay, 1, 0)
        + jnp.where(is_s, G * N_COL - 1 + G * G * (NG - 1 - a), 1)
        + jnp.where(half < a, 1, 0)
        + jnp.where(half + 2 < a, 1, 0)
    )

    lane = lax.broadcasted_iota(jnp.int32, (RHS, RMAX), 1)
    loads[3].wait()
    live = [lane < rank_s[0, b] for b in range(2)]

    with jax.named_scope("up"):
        loads[1].wait()
        loads[2].wait()
        loads[0].wait()
        up = nn(cx_v[...], bt_v[...])
        pieces = [up[:, m * BLK:(m + 1) * BLK] for m in range(BB)]
        ids = [jnp.full((RHS, BLK), blocks_s[0, m], jnp.int32) for m in range(BB)]

        @pl.loop(0, NT)
        def _(r):
            for q in range(QB):
                block = jnp.zeros((RHS, BLK), F32)
                for m in range(BB):
                    block = block + jnp.where(ids[m] == r * (QB) + q, pieces[m], 0.0)
                childp[r, :, q * BLK:(q + 1) * BLK] = block

    loads[4].wait()
    loads[5].wait()
    slot = div(a, 2)
    owner = (half == mod(a, 2)) & (jcol < ii)
    t_idx = div(ii * (ii - 1), 2) + jcol
    own_tile = jnp.where(owner & is_s, t_idx, -1)

    @pl.when(owner)
    def _():
        us[...] = u_v[slot].astype(F32)
        wide = lax.broadcasted_iota(jnp.int32, (TILE, RMAX), 1)
        vs[...] = jnp.where(wide < rank_s[0, slot], v_v[slot].astype(F32), 0.0)

    @pl.when(owner & is_s)
    def _():
        urx[t_idx] = us[...]
        vrx[t_idx] = vs[...]

    with jax.named_scope("bar"):
        pl.semaphore_wait(bar, greeted)

    def child_copy(k):
        peer = mod(row + k, N_ROW)
        return remote(childp.at[peer], childrx.at[k], csend.at[k], crecv.at[k], peer, col)

    @pl.loop(1, N_ROW)
    def _(k):
        child_copy(k).start()

    def v_copy():
        return remote(vs, vrx.at[t_idx], tsend.at[0], trecv.at[0, t_idx], srow, scol)

    def u_copy():
        return remote(us, urx.at[t_idx], tsend.at[1], trecv.at[1, t_idx], srow, scol)

    def relay_in():
        return remote(
            us, urelay, tsend.at[1], rrecv.at[0], jnp.int32(RELAY[0]), jnp.int32(RELAY[1])
        )

    def relay_out():
        t = pair(*SOURCE)
        return remote(urelay, urx.at[t], rsend.at[0], trecv.at[1, t], srow, scol)

    sends_tile = owner & jnp.logical_not(is_s)
    sends_u = sends_tile & jnp.logical_not(is_source)
    pl.when(sends_tile)(lambda: v_copy().start())
    pl.when(sends_u)(lambda: u_copy().start())
    pl.when(is_source)(lambda: relay_in().start())

    with jax.named_scope("child_wait"):
        @pl.loop(1, N_ROW)
        def _(k):
            child_copy(k).wait_recv()

        total = childp[row]
        for k in range(1, N_ROW):
            total = total + childrx[k]
        rowmsg[...] = total

    with jax.named_scope("fwd_row"):
        for b in range(2):
            @pl.when(col + N_COL * b < G * a)
            def _():
                remote(xs.at[0], xrx.at[b], xsend.at[0], xrecv.at[b], srow, scol).wait_recv()
                p = nn(xrx[b].astype(BF16), v_v[b])
                p = jnp.where(live[b], p, 0.0).astype(BF16)
                rowmsg[...] += nn(p, u_v[b])

    def row_copy():
        return remote(
            rowmsg, srx.at[ii, col], msend.at[0], srecv.at[ii, col], srow, scol
        )

    @pl.when(is_s)
    def _():
        srx[ii, col] = rowmsg[...]

    @pl.when(jnp.logical_not(is_s))
    def _():
        row_copy().start()

    @pl.when(is_relay)
    def _():
        relay_in().wait_recv()
        relay_out().start()

    loads[6].wait()
    loads[7].wait()

    def turn():
        with jax.named_scope("turn"):
            for t in range(G * (G - 1) // 2):
                utin[t] = urx[t].T.astype(BF16)
                vtin[t] = vrx[t].T.astype(BF16)
            for jj in range(G):
                dt[jj] = d_v[jj].T

    def x_copy(jj, da, i2):
        return remote(
            xs.at[jj], xrx.at[slot], xsend.at[(da * G + jj) * G + i2], xrecv.at[slot],
            G * (a + da) + i2, ours + jj,
        )

    @pl.when(is_s)
    def _():
        with jax.named_scope("tiles_wait"):
            for t in range(G * (G - 1) // 2):
                @pl.when(own_tile != t)
                def _():
                    remote(vs, vrx.at[t], tsend.at[0], trecv.at[0, t], srow, scol).wait_recv()
                    remote(us, urx.at[t], tsend.at[1], trecv.at[1, t], srow, scol).wait_recv()

                vbf[t] = vrx[t].astype(BF16)
                ubf[t] = urx[t].astype(BF16)
        pl.when(a == NG - 1)(turn)
        inner = [None] * G
        for jj in range(G):
            with jax.named_scope(f"s_fwd_wait{jj}"):
                for c in range(N_COL):
                    def wait_row():
                        remote(
                            rowmsg, srx.at[jj, c], msend.at[0], srecv.at[jj, c], srow, scol
                        ).wait_recv()

                    pl.when((srel != jj) | (col != c))(wait_row)
            tot = srx[jj, 0]
            for c in range(1, N_COL):
                tot = tot + srx[jj, c]
            if inner[jj] is not None:
                tot = tot + inner[jj]
            right = rhs_v[:, jj * TILE:(jj + 1) * TILE].astype(F32) - tot
            x = folded(nn(two_halves(right), d_v[jj]))
            xs[jj] = x

            @pl.when(a + 1 < NG)
            def _():
                for i2 in range(G):
                    x_copy(jj, 1, i2).start()

            xb = x.astype(BF16)
            for mm in range(jj + 1, G):
                t = pair(mm, jj)
                part = nn(nn(xb, vbf[t]).astype(BF16), ubf[t])
                inner[mm] = part if inner[mm] is None else inner[mm] + part
        for da in range(2, NG):
            @pl.when(a + da < NG)
            def _():
                for i2 in range(G):
                    for jj in range(G):
                        x_copy(jj, da, i2).start()
        pl.when(a < NG - 1)(turn)

    with jax.named_scope("turn2"):
        for b in range(2):
            @pl.when(col + N_COL * b < G * a)
            def _():
                ut[b] = u_v[b].T
                vt[b] = v_v[b].T

    def z_tile(i):
        return zfull.at[pl.ds(QB * i, QB)]

    def z_copy(jj, k):
        c = mod(G - ours + k, N_COL)
        return c, remote(
            zs.at[jj], z_tile(G * a + jj), zsend.at[jj, k], zrecv.at[0], G * a + jj, c
        )

    @pl.when(is_s)
    def _():
        inner = [None] * G
        for jj in reversed(range(G)):
            with jax.named_scope(f"s_bwd_wait{jj}"):
                tacc[...] = xs[jj]
                for da in reversed(range(1, NG)):
                    @pl.when(a + da < NG)
                    def _():
                        for i2 in range(G):
                            n = (da - 1) * G + i2
                            remote(
                                bmsg.at[0], brx.at[jj, n], bsend.at[0], brecv.at[jj, n],
                                srow, scol,
                            ).wait_recv()
                        n = (da - 1) * G
                        part = (brx[jj, n] + brx[jj, n + 1]) + (brx[jj, n + 2] + brx[jj, n + 3])
                        tacc[...] -= part
            left = tacc[...]
            if inner[jj] is not None:
                left = left - inner[jj]
            z = folded(nn(two_halves(left), dt[jj]))
            for q in range(QB):
                zs[jj, q] = z[:, q * BLK:(q + 1) * BLK]
                zfull[QB * (G * a + jj) + q] = z[:, q * BLK:(q + 1) * BLK]
            for k in range(N_COL):
                c, copy = z_copy(jj, k)
                pl.when((srel != jj) | (c != col))(copy.start)
            zb = z.astype(BF16)
            for mm in range(jj):
                t = pair(jj, mm)
                part = nn(nn(zb, utin[t]).astype(BF16), vtin[t])
                inner[mm] = part if inner[mm] is None else inner[mm] + part

    @pl.when(jnp.logical_not(is_s))
    def _():
        with jax.named_scope("z_wait"):
            remote(zs.at[0], z_tile(row), zsend.at[0, 0], zrecv.at[0], srow, scol).wait_recv()

    def back_copy(b):
        g = half + 2 * b
        n = (a - g - 1) * G + ii
        return remote(
            bmsg.at[b], brx.at[jcol, n], bsend.at[b], brecv.at[jcol, n], *solver_of(g)
        )

    mine = jnp.concatenate([zfull[QB * row + q] for q in range(QB)], axis=1)
    for b in reversed(range(2)):
        @pl.when(col + N_COL * b < G * a)
        def _():
            q = nn(mine.astype(BF16), ut[b])
            q = jnp.where(live[b], q, 0.0).astype(BF16)
            bmsg[b] = nn(q, vt[b])
            back_copy(b).start()

    def gather_copy(k):
        peer = mod(row + k, N_ROW)
        return remote(z_tile(row), z_tile(row), gsend.at[k], grecv.at[k], peer, col)

    @pl.loop(1, N_ROW)
    def _(k):
        gather_copy(k).start()

    wide = zfull[QB * row + div(col, 2)]
    root_out[...] = jnp.where(mod(col, 2) == 0, wide[:, :HALF], wide[:, HALF:])

    with jax.named_scope("gather_wait"):
        @pl.loop(1, N_ROW)
        def _(k):
            source = mod(row + N_ROW - k, N_ROW)
            remote(
                z_tile(source), z_tile(source), gsend.at[k], grecv.at[k], source, col
            ).wait_recv()

    with jax.named_scope("final"):
        loads[8].wait()
        parts = [zfull[blocks_s[0, m]] for m in range(BB)]
        gathered = jnp.concatenate(parts, axis=1).astype(BF16)
        returned = nt(gathered, bt_v[...])
        child_out[0] = cx_v[...].astype(F32) - folded(nn(two_halves(returned), ci_v[...]))

    @pl.loop(1, N_ROW)
    def _(k):
        child_copy(k).wait_send()
        gather_copy(k).wait_send()

    pl.when(sends_tile)(lambda: v_copy().wait_send())
    pl.when(sends_u)(lambda: u_copy().wait_send())
    pl.when(is_source)(lambda: relay_in().wait_send())
    pl.when(is_relay)(lambda: relay_out().wait_send())

    @pl.when(jnp.logical_not(is_s))
    def _():
        row_copy().wait_send()

    for b in range(2):
        @pl.when(col + N_COL * b < G * a)
        def _():
            back_copy(b).wait_send()

    @pl.when(is_s)
    def _():
        for da in range(1, NG):
            @pl.when(a + da < NG)
            def _():
                for i2 in range(G):
                    for jj in range(G):
                        x_copy(jj, da, i2).wait_send()
        for jj in range(G):
            for k in range(N_COL):
                c, copy = z_copy(jj, k)
                pl.when((srel != jj) | (c != col))(copy.wait_send)


def per_device(
    root_rhs, diag_inv, tile_u, tile_v, tile_rank, child_x, border_t, child_inv, child_blocks
):
    vmem = pl.BlockSpec(memory_space=pltpu.VMEM)
    hbm = pl.BlockSpec(memory_space=pltpu.HBM)
    dma = pltpu.SemaphoreType.DMA
    pairs = G * (G - 1) // 2
    wide = (RHS, TILE)
    return pl.pallas_call(
        kernel,
        out_shape=(
            jax.ShapeDtypeStruct((RHS, HALF), F32),
            jax.ShapeDtypeStruct((1, RHS, TILE), F32),
        ),
        in_specs=[hbm] * 9,
        out_specs=(vmem, vmem),
        scratch_shapes=[
            pltpu.VMEM((RHS, G * TILE), BF16),
            pltpu.VMEM(wide, BF16),
            pltpu.SMEM((1, BB), jnp.int32),
            pltpu.SMEM((1, 2), jnp.int32),
            pltpu.VMEM((RMAX, TILE), F32),
            pltpu.VMEM((G, TILE, TILE), BF16),
            pltpu.VMEM((2, TILE, RMAX), BF16),
            pltpu.VMEM((2, RMAX, TILE), BF16),
            pltpu.VMEM((pairs, TILE, RMAX), BF16),
            pltpu.VMEM((pairs, RMAX, TILE), BF16),
            pltpu.VMEM((TILE, BB * BLK), BF16),
            pltpu.VMEM((TILE, TILE), BF16),
            pltpu.VMEM((2, RMAX, TILE), BF16),
            pltpu.VMEM((2, TILE, RMAX), BF16),
            pltpu.VMEM((G, TILE, TILE), BF16),
            pltpu.VMEM((RMAX, TILE), F32),
            pltpu.VMEM((TILE, RMAX), F32),
            pltpu.VMEM((pairs, RMAX, TILE), F32),
            pltpu.VMEM((pairs, TILE, RMAX), F32),
            pltpu.VMEM((pairs, RMAX, TILE), BF16),
            pltpu.VMEM((pairs, TILE, RMAX), BF16),
            pltpu.VMEM((NT, *wide), F32),
            pltpu.VMEM((N_ROW, *wide), F32),
            pltpu.VMEM((2, *wide), F32),
            pltpu.VMEM(wide, F32),
            pltpu.VMEM((G, N_COL, *wide), F32),
            pltpu.VMEM((G, *wide), F32),
            pltpu.VMEM((NT * QB, RHS, BLK), F32),
            pltpu.VMEM((G, QB, RHS, BLK), F32),
            pltpu.VMEM((2, *wide), F32),
            pltpu.VMEM((G, (NG - 1) * G, *wide), F32),
            pltpu.VMEM(wide, F32),
            dma((9,)),
            dma((N_ROW,)),
            dma((N_ROW,)),
            dma((2,)),
            dma((2, pairs)),
            dma((1,)),
            dma((G, N_COL)),
            dma((NG * G * G,)),
            dma((2,)),
            dma((G, N_COL)),
            dma((1,)),
            dma((2,)),
            dma((G, (NG - 1) * G)),
            dma((N_ROW,)),
            dma((N_ROW,)),
            dma((1,)),
            dma((1,)),
        ],
        compiler_params=pltpu.CompilerParams(
            collective_id=0, has_side_effects=True, vmem_limit_bytes=66_950_000
        ),
    )(
        root_rhs, child_x, child_blocks, tile_rank, diag_inv, tile_u, tile_v, border_t, child_inv
    )


def solution(mesh):
    both = ("row", "col")
    tiles = P("row", "col", None, None, None, None)
    in_specs = (
        P(),
        P(),
        tiles,
        tiles,
        P("row", "col", None, None),
        P(both, None, None),
        P(both, None, None),
        P(both, None, None),
        P(both, None),
    )
    out_specs = (P(None, both), P(both, None, None))
    return jax.shard_map(
        per_device, mesh=mesh, in_specs=in_specs, out_specs=out_specs, check_vma=False
    )
```

```python
import jax
import jax.numpy as jnp
from jax import lax
from jax.experimental import pallas as pl
from jax.experimental.pallas import tpu as pltpu
from jax.sharding import PartitionSpec as P

MESH = pl.DeviceIdType.MESH
F32 = jnp.float32
BF16 = jnp.bfloat16
NT = 16
TILE = 512
RHS = 8
RMAX = 128
BLK = 128
BB = 8
N_ROW = 16
N_COL = 8
G = 4
NG = NT // G
SOLVER_ROW = (3, 3, 2, 0)
SOLVER_COL = (1, 5, 7, 3)
FAR_FIRST = (
    (2, 2), (3, 2), (0, 2), (2, 3), (3, 3), (0, 1), (2, 1), (3, 1), (0, 3),
    (1, 2), (3, 0), (1, 3), (1, 1), (2, 0), (1, 0),
)
SOURCE = (2, 0)
RELAY = (3, 3)
HALF = TILE // N_COL
QB = TILE // BLK


def div(x, n):
    return lax.div(x, jnp.int32(n))


def mod(x, n):
    return lax.rem(x, jnp.int32(n))


def pick(table, group):
    if isinstance(group, int):
        return jnp.int32(table[group])
    value = jnp.int32(table[-1])
    for g in range(len(table) - 1):
        value = jnp.where(group == g, jnp.int32(table[g]), value)
    return value


def solver_of(group):
    return G * group + pick(SOLVER_ROW, group), pick(SOLVER_COL, group)


def pair(i, j):
    return i * (i - 1) // 2 + j


def nn(a, b):
    return lax.dot_general(a, b, (((1,), (0,)), ((), ())), preferred_element_type=F32)


def nt(a, b):
    return lax.dot_general(a, b, (((1,), (1,)), ((), ())), preferred_element_type=F32)


def two_halves(t):
    hi = t.astype(BF16).astype(F32)
    return jnp.concatenate([hi, t - hi], axis=0).astype(BF16)


def folded(r):
    return r[:RHS] + r[RHS:]


def kernel(
    rhs_hbm, cx_hbm, blocks_hbm, rank_hbm, diag_hbm, u_hbm, v_hbm, bt_hbm, ci_hbm,
    root_out, child_out,
    rhs_v, cx_v, blocks_s, rank_s, urelay, dt, ut, vt, utin,
    bt_v, ci_v, u_v, v_v, d_v, us, vs, urx, vrx, wf, wb, vbf,
    childp, childrx, xrx, rowmsg, srx, xs, zfull, zs, bmsg, brx, tacc,
    lsem, csend, crecv, tsend, trecv, msend, srecv, xsend, xrecv,
    zsend, zrecv, bsend, brecv, gsend, grecv, rsend, rrecv,
):
    row = lax.axis_index("row")
    col = lax.axis_index("col")
    a = div(row, G)
    ii = mod(row, G)
    half = div(col, G)
    jcol = mod(col, G)
    srow, scol = solver_of(a)
    srel = srow - G * a
    is_s = (row == srow) & (col == scol)
    ours = G * mod(a, 2)
    is_source = (row == SOURCE[0]) & (col == SOURCE[1])
    is_relay = (row == RELAY[0]) & (col == RELAY[1])

    width = G * TILE
    loads = [
        pltpu.make_async_copy(bt_hbm.at[0], bt_v, lsem.at[0]),
        pltpu.make_async_copy(cx_hbm.at[0], cx_v, lsem.at[1]),
        pltpu.make_async_copy(blocks_hbm, blocks_s, lsem.at[2]),
        pltpu.make_async_copy(rank_hbm.at[0, 0], rank_s, lsem.at[3]),
        pltpu.make_async_copy(u_hbm.at[0, 0, 0], u_v, lsem.at[4]),
        pltpu.make_async_copy(v_hbm.at[0, 0, 0], v_v, lsem.at[5]),
        pltpu.make_async_copy(
            rhs_hbm.at[:, pl.ds(pl.multiple_of(width * a, width), width)], rhs_v, lsem.at[6]
        ),
        pltpu.make_async_copy(diag_hbm.at[pl.ds(G * a, G)], d_v, lsem.at[7]),
        pltpu.make_async_copy(ci_hbm.at[0], ci_v, lsem.at[8]),
    ]
    for load in loads:
        load.start()

    def remote(src, dst, send, recv, r, c):
        return pltpu.make_async_remote_copy(
            src_ref=src, dst_ref=dst, send_sem=send, recv_sem=recv,
            device_id=(r, c), device_id_type=MESH,
        )

    bar = pltpu.get_barrier_semaphore()

    def signal(r, c):
        pl.semaphore_signal(bar, inc=1, device_id=(r, c), device_id_type=MESH)

    for k in range(1, N_ROW):
        signal(mod(row + k, N_ROW), col)

    @pl.when(jnp.logical_not(is_s))
    def _():
        signal(srow, scol)

    for b in range(2):
        @pl.when(half + 2 * b < a)
        def _():
            signal(*solver_of(half + 2 * b))

    @pl.when(is_s)
    def _():
        me = ii * N_COL + col
        for k in range(1, G * N_COL):
            other = mod(me + k, G * N_COL)
            signal(G * a + div(other, N_COL), mod(other, N_COL))
        for da in range(1, NG):
            @pl.when(a + da < NG)
            def _():
                for n in range(G * G):
                    signal(G * (a + da) + n // G, ours + n % G)

    @pl.when(is_source)
    def _():
        signal(jnp.int32(RELAY[0]), jnp.int32(RELAY[1]))

    @pl.when(is_relay)
    def _():
        signal(jnp.int32(SOURCE[0]), jnp.int32(SOURCE[1]))

    greeted = (
        N_ROW - 1
        + jnp.where(is_source | is_relay, 1, 0)
        + jnp.where(is_s, G * N_COL - 1 + G * G * (NG - 1 - a), 1)
        + jnp.where(half < a, 1, 0)
        + jnp.where(half + 2 < a, 1, 0)
    )

    lane = lax.broadcasted_iota(jnp.int32, (RHS, RMAX), 1)
    loads[3].wait()
    live = [lane < rank_s[0, b] for b in range(2)]

    with jax.named_scope("up"):
        loads[1].wait()
        loads[2].wait()
        loads[0].wait()
        up = nn(cx_v[...], bt_v[...])
        pieces = [up[:, m * BLK:(m + 1) * BLK] for m in range(BB)]
        ids = [jnp.full((RHS, BLK), blocks_s[0, m], jnp.int32) for m in range(BB)]

        @pl.loop(0, NT)
        def _(r):
            for q in range(QB):
                block = jnp.zeros((RHS, BLK), F32)
                for m in range(BB):
                    block = block + jnp.where(ids[m] == r * (QB) + q, pieces[m], 0.0)
                childp[r, :, q * BLK:(q + 1) * BLK] = block

    loads[4].wait()
    loads[5].wait()
    slot = div(a, 2)
    owner = (half == mod(a, 2)) & (jcol < ii)
    t_idx = div(ii * (ii - 1), 2) + jcol
    own_tile = jnp.where(owner & is_s, t_idx, -1)

    @pl.when(owner)
    def _():
        us[...] = u_v[slot].astype(F32)
        wide = lax.broadcasted_iota(jnp.int32, (TILE, RMAX), 1)
        vs[...] = jnp.where(wide < rank_s[0, slot], v_v[slot].astype(F32), 0.0)

    @pl.when(owner & is_s)
    def _():
        urx[t_idx] = us[...]
        vrx[t_idx] = vs[...]

    with jax.named_scope("bar"):
        pl.semaphore_wait(bar, greeted)

    def peer_row(k, sign=1):
        dy, dz = FAR_FIRST[k - 1]
        return G * mod(a + G + sign * dy, NG) + mod(ii + G + sign * dz, G)

    def child_copy(k):
        peer = peer_row(k)
        return remote(childp.at[peer], childrx.at[k - 1], csend.at[0], crecv.at[0], peer, col)

    def all_children():
        every = pl.ds(0, N_ROW - 1)
        return remote(
            childp.at[every], childrx.at[every], csend.at[0], crecv.at[0], srow, scol
        )

    for k in range(1, N_ROW):
        child_copy(k).start()

    def v_copy():
        return remote(vs, vrx.at[t_idx], tsend.at[0], trecv.at[0, t_idx], srow, scol)

    def u_copy():
        return remote(us, urx.at[t_idx], tsend.at[1], trecv.at[1, t_idx], srow, scol)

    def relay_in():
        return remote(
            us, urelay, tsend.at[1], rrecv.at[0], jnp.int32(RELAY[0]), jnp.int32(RELAY[1])
        )

    def relay_out():
        t = pair(*SOURCE)
        return remote(urelay, urx.at[t], rsend.at[0], trecv.at[1, t], srow, scol)

    sends_tile = owner & jnp.logical_not(is_s)
    sends_u = sends_tile & jnp.logical_not(is_source)
    pl.when(sends_tile)(lambda: v_copy().start())
    pl.when(sends_u)(lambda: u_copy().start())
    pl.when(is_source)(lambda: relay_in().start())

    with jax.named_scope("child_wait"):
        all_children().wait_recv()
        total = childp[row]
        for k in range(N_ROW - 1):
            total = total + childrx[k]
        rowmsg[...] = total

    tiles = [(i, j) for i in range(G) for j in range(i)]

    def turn():
        with jax.named_scope("turn"):
            for jj in range(G):
                dt[jj] = d_v[jj].T
            for i, j in tiles:
                t = pair(i, j)
                utin[t] = urx[t].T.astype(BF16)
                wb[t] = nn(vrx[t].T.astype(BF16), dt[j]).astype(BF16)

    loads[7].wait()

    @pl.when(is_s)
    def _():
        with jax.named_scope("tiles_wait"):
            for i, j in tiles:
                t = pair(i, j)

                @pl.when(own_tile != t)
                def _():
                    remote(vs, vrx.at[t], tsend.at[0], trecv.at[0, t], srow, scol).wait_recv()
                    remote(us, urx.at[t], tsend.at[1], trecv.at[1, t], srow, scol).wait_recv()

                vbf[t] = vrx[t].astype(BF16)
                wf[t] = nn(urx[t].astype(BF16), d_v[i]).astype(BF16)
        pl.when(a == NG - 1)(turn)

    with jax.named_scope("turn2"):
        for b in range(2):
            @pl.when(col + N_COL * b < G * a)
            def _():
                ut[b] = u_v[b].T
                vt[b] = v_v[b].T

    with jax.named_scope("fwd_row"):
        for b in range(2):
            @pl.when(col + N_COL * b < G * a)
            def _():
                remote(xs.at[0], xrx.at[b], xsend.at[0], xrecv.at[b], srow, scol).wait_recv()
                p = nn(xrx[b].astype(BF16), v_v[b])
                p = jnp.where(live[b], p, 0.0).astype(BF16)
                rowmsg[...] += nn(p, u_v[b])

    def row_copy():
        return remote(
            rowmsg, srx.at[ii, col], msend.at[0], srecv.at[ii], srow, scol
        )

    @pl.when(is_s)
    def _():
        srx[ii, col] = rowmsg[...]

    @pl.when(jnp.logical_not(is_s))
    def _():
        row_copy().start()

    @pl.when(is_relay)
    def _():
        relay_in().wait_recv()
        relay_out().start()

    loads[6].wait()

    def x_copy(jj, da, i2):
        return remote(
            xs.at[jj], xrx.at[slot], xsend.at[da - 1], xrecv.at[slot],
            G * (a + da) + i2, ours + jj,
        )

    @pl.when(is_s)
    def _():
        inner = [None] * G
        for jj in range(G):
            with jax.named_scope(f"s_fwd_wait{jj}"):
                def wait_row(count):
                    slots = srx.at[jj, pl.ds(0, count)]
                    remote(
                        slots, slots, msend.at[0], srecv.at[jj], srow, scol
                    ).wait_recv()

                pl.when(srel != jj)(lambda: wait_row(N_COL))
                pl.when(srel == jj)(lambda: wait_row(N_COL - 1))
            tot = srx[jj, 0]
            for c in range(1, N_COL):
                tot = tot + srx[jj, c]
            right = rhs_v[:, jj * TILE:(jj + 1) * TILE].astype(F32) - tot
            x = folded(nn(two_halves(right), d_v[jj]))
            if inner[jj] is not None:
                x = x - inner[jj]
            xs[jj] = x

            @pl.when(a + 1 < NG)
            def _():
                for i2 in range(G):
                    x_copy(jj, 1, i2).start()

            xb = x.astype(BF16)
            for mm in range(jj + 1, G):
                t = pair(mm, jj)
                part = nn(nn(xb, vbf[t]).astype(BF16), wf[t])
                inner[mm] = part if inner[mm] is None else inner[mm] + part
        for da in range(2, NG):
            @pl.when(a + da < NG)
            def _():
                for i2 in range(G):
                    for jj in range(G):
                        x_copy(jj, da, i2).start()
        pl.when(a < NG - 1)(turn)

    all_children().wait_send()
    pl.when(sends_tile)(lambda: v_copy().wait_send())
    pl.when(sends_u)(lambda: u_copy().wait_send())
    pl.when(is_source)(lambda: relay_in().wait_send())
    pl.when(is_relay)(lambda: relay_out().wait_send())
    pl.when(jnp.logical_not(is_s))(lambda: row_copy().wait_send())

    def z_tile(i):
        return zfull.at[pl.ds(QB * i, QB)]

    def z_copy(jj, k):
        c = mod(G - ours + k, N_COL)
        return c, remote(
            zs.at[jj], z_tile(G * a + jj), zsend.at[jj], zrecv.at[0], G * a + jj, c
        )

    @pl.when(is_s)
    def _():
        inner = [None] * G
        for jj in reversed(range(G)):
            with jax.named_scope(f"s_bwd_wait{jj}"):
                tacc[...] = xs[jj]
                for da in reversed(range(1, NG)):
                    @pl.when(a + da < NG)
                    def _():
                        slots = brx.at[jj, pl.ds((da - 1) * G, G)]
                        remote(
                            slots, slots, bsend.at[0], brecv.at[jj, da - 1], srow, scol
                        ).wait_recv()
                        n = (da - 1) * G
                        part = (brx[jj, n] + brx[jj, n + 1]) + (brx[jj, n + 2] + brx[jj, n + 3])
                        tacc[...] -= part
            z = folded(nn(two_halves(tacc[...]), dt[jj]))
            if inner[jj] is not None:
                z = z - inner[jj]
            for q in range(QB):
                zs[jj, q] = z[:, q * BLK:(q + 1) * BLK]
                zfull[QB * (G * a + jj) + q] = z[:, q * BLK:(q + 1) * BLK]
            for k in range(N_COL):
                c, copy = z_copy(jj, k)
                pl.when((srel != jj) | (c != col))(copy.start)
            zb = z.astype(BF16)
            for mm in range(jj):
                t = pair(jj, mm)
                part = nn(nn(zb, utin[t]).astype(BF16), wb[t])
                inner[mm] = part if inner[mm] is None else inner[mm] + part

    @pl.when(jnp.logical_not(is_s))
    def _():
        with jax.named_scope("z_wait"):
            remote(zs.at[0], z_tile(row), zsend.at[0], zrecv.at[0], srow, scol).wait_recv()

    def back_copy(b):
        g = half + 2 * b
        n = (a - g - 1) * G + ii
        return remote(
            bmsg.at[b], brx.at[jcol, n], bsend.at[b], brecv.at[jcol, a - g - 1], *solver_of(g)
        )

    mine = jnp.concatenate([zfull[QB * row + q] for q in range(QB)], axis=1)
    for b in reversed(range(2)):
        @pl.when(col + N_COL * b < G * a)
        def _():
            q = nn(mine.astype(BF16), ut[b])
            q = jnp.where(live[b], q, 0.0).astype(BF16)
            bmsg[b] = nn(q, vt[b])
            back_copy(b).start()

    def gather_copy(k):
        peer = peer_row(k)
        return remote(z_tile(row), z_tile(row), gsend.at[0], grecv.at[0], peer, col)

    def all_gathered():
        every = zfull.at[pl.ds(0, QB * (N_ROW - 1))]
        return remote(every, every, gsend.at[0], grecv.at[0], srow, scol)

    for k in range(1, N_ROW):
        gather_copy(k).start()

    wide = zfull[QB * row + div(col, 2)]
    root_out[...] = jnp.where(mod(col, 2) == 0, wide[:, :HALF], wide[:, HALF:])

    for b in range(2):
        @pl.when(col + N_COL * b < G * a)
        def _():
            back_copy(b).wait_send()

    @pl.when(is_s)
    def _():
        for da in range(1, NG):
            @pl.when(a + da < NG)
            def _():
                slots = brx.at[:, pl.ds(0, G)]
                remote(slots, slots, xsend.at[da - 1], xrecv.at[0], srow, scol).wait_send()
        for jj in range(G):
            def wait_z(count):
                slots = srx.at[jj, pl.ds(0, count)]
                remote(slots, slots, zsend.at[jj], zrecv.at[0], srow, scol).wait_send()

            pl.when(srel != jj)(lambda: wait_z(N_COL))
            pl.when(srel == jj)(lambda: wait_z(N_COL - 1))

    with jax.named_scope("gather_wait"):
        all_gathered().wait_recv()

    with jax.named_scope("final"):
        loads[8].wait()
        parts = [zfull[blocks_s[0, m]] for m in range(BB)]
        gathered = jnp.concatenate(parts, axis=1).astype(BF16)
        returned = nt(gathered, bt_v[...])
        child_out[0] = cx_v[...].astype(F32) - folded(nn(two_halves(returned), ci_v[...]))

    all_gathered().wait_send()


def per_device(
    root_rhs, diag_inv, tile_u, tile_v, tile_rank, child_x, border_t, child_inv, child_blocks
):
    vmem = pl.BlockSpec(memory_space=pltpu.VMEM)
    hbm = pl.BlockSpec(memory_space=pltpu.HBM)
    dma = pltpu.SemaphoreType.DMA
    pairs = G * (G - 1) // 2
    wide = (RHS, TILE)
    return pl.pallas_call(
        kernel,
        out_shape=(
            jax.ShapeDtypeStruct((RHS, HALF), F32),
            jax.ShapeDtypeStruct((1, RHS, TILE), F32),
        ),
        in_specs=[hbm] * 9,
        out_specs=(vmem, vmem),
        scratch_shapes=[
            pltpu.VMEM((RHS, G * TILE), BF16),
            pltpu.VMEM(wide, BF16),
            pltpu.SMEM((1, BB), jnp.int32),
            pltpu.SMEM((1, 2), jnp.int32),
            pltpu.VMEM((RMAX, TILE), F32),
            pltpu.VMEM((G, TILE, TILE), BF16),
            pltpu.VMEM((2, TILE, RMAX), BF16),
            pltpu.VMEM((2, RMAX, TILE), BF16),
            pltpu.VMEM((pairs, TILE, RMAX), BF16),
            pltpu.VMEM((TILE, BB * BLK), BF16),
            pltpu.VMEM((TILE, TILE), BF16),
            pltpu.VMEM((2, RMAX, TILE), BF16),
            pltpu.VMEM((2, TILE, RMAX), BF16),
            pltpu.VMEM((G, TILE, TILE), BF16),
            pltpu.VMEM((RMAX, TILE), F32),
            pltpu.VMEM((TILE, RMAX), F32),
            pltpu.VMEM((pairs, RMAX, TILE), F32),
            pltpu.VMEM((pairs, TILE, RMAX), F32),
            pltpu.VMEM((pairs, RMAX, TILE), BF16),
            pltpu.VMEM((pairs, RMAX, TILE), BF16),
            pltpu.VMEM((pairs, TILE, RMAX), BF16),
            pltpu.VMEM((NT, *wide), F32),
            pltpu.VMEM((N_ROW, *wide), F32),
            pltpu.VMEM((2, *wide), F32),
            pltpu.VMEM(wide, F32),
            pltpu.VMEM((G, N_COL, *wide), F32),
            pltpu.VMEM((G, *wide), F32),
            pltpu.VMEM((NT * QB, RHS, BLK), F32),
            pltpu.VMEM((G, QB, RHS, BLK), F32),
            pltpu.VMEM((2, *wide), F32),
            pltpu.VMEM((G, (NG - 1) * G, *wide), F32),
            pltpu.VMEM(wide, F32),
            dma((9,)),
            dma((1,)),
            dma((1,)),
            dma((2,)),
            dma((2, pairs)),
            dma((1,)),
            dma((G,)),
            dma((NG - 1,)),
            dma((2,)),
            dma((G,)),
            dma((1,)),
            dma((2,)),
            dma((G, NG - 1)),
            dma((1,)),
            dma((1,)),
            dma((1,)),
            dma((1,)),
        ],
        compiler_params=pltpu.CompilerParams(
            collective_id=0, has_side_effects=True, vmem_limit_bytes=48_000_000
        ),
    )(
        *(
            pltpu.with_memory_space_constraint(array, pltpu.HBM)
            for array in (
                root_rhs, child_x, child_blocks, tile_rank, diag_inv,
                tile_u, tile_v, border_t, child_inv,
            )
        )
    )


def solution(mesh):
    both = ("row", "col")
    tiles = P("row", "col", None, None, None, None)
    in_specs = (
        P(),
        P(),
        tiles,
        tiles,
        P("row", "col", None, None),
        P(both, None, None),
        P(both, None, None),
        P(both, None, None),
        P(both, None),
    )
    out_specs = (P(None, both), P(both, None, None))
    return jax.shard_map(
        per_device, mesh=mesh, in_specs=in_specs, out_specs=out_specs, check_vma=False
    )
```

```python
import jax
import jax.numpy as jnp
from jax import lax
from jax.experimental import pallas as pl
from jax.experimental.pallas import tpu as pltpu
from jax.sharding import PartitionSpec as P

MESH = pl.DeviceIdType.MESH
F32 = jnp.float32
BF16 = jnp.bfloat16
NT = 16
TILE = 512
RHS = 8
RMAX = 128
BLK = 128
BB = 8
N_ROW = 16
N_COL = 8
G = 4
NG = NT // G
SOLVER_ROW = (3, 3, 2, 0)
SOLVER_COL = (1, 3, 3, 3)
JOIN = 3
FAR_FIRST = (
    (2, 2), (3, 2), (0, 2), (2, 3), (3, 3), (0, 1), (2, 1), (3, 1), (0, 3),
    (1, 2), (3, 0), (1, 3), (1, 1), (2, 0), (1, 0),
)
SOURCE = (2, 0)
RELAY = (3, 3)
HALF = TILE // N_COL
QB = TILE // BLK


def div(x, n):
    return lax.div(x, jnp.int32(n))


def mod(x, n):
    return lax.rem(x, jnp.int32(n))


def pick(table, group):
    if isinstance(group, int):
        return jnp.int32(table[group])
    value = jnp.int32(table[-1])
    for g in range(len(table) - 1):
        value = jnp.where(group == g, jnp.int32(table[g]), value)
    return value


def solver_of(group):
    return G * group + pick(SOLVER_ROW, group), pick(SOLVER_COL, group)


def pair(i, j):
    return i * (i - 1) // 2 + j


def nn(a, b):
    return lax.dot_general(a, b, (((1,), (0,)), ((), ())), preferred_element_type=F32)


def nt(a, b):
    return lax.dot_general(a, b, (((1,), (1,)), ((), ())), preferred_element_type=F32)


def two_halves(t):
    hi = t.astype(BF16).astype(F32)
    return jnp.concatenate([hi, t - hi], axis=0).astype(BF16)


def folded(r):
    return r[:RHS] + r[RHS:]


def kernel(
    rhs_hbm, cx_hbm, blocks_hbm, rank_hbm, diag_hbm, u_hbm, v_hbm, bt_hbm, ci_hbm,
    root_out, child_out,
    rhs_v, cx_v, blocks_s, rank_s, urelay, dt, ut, vt, utin,
    vjoin, ujoin, vj, uj, vjt, ujt, xjoin, bjoin,
    bt_v, ci_v, u_v, v_v, d_v, us, vs, urx, vrx, wf, wb, vbf,
    childp, childrx, xrx, rowmsg, srx, xs, zfull, zs, bmsg, brx, tacc,
    lsem, csend, crecv, tsend, trecv, msend, srecv, xsend, xrecv,
    zsend, zrecv, bsend, brecv, gsend, grecv, rsend, rrecv, jtile, xjrecv, bjsend,
):
    row = lax.axis_index("row")
    col = lax.axis_index("col")
    a = div(row, G)
    ii = mod(row, G)
    half = div(col, G)
    jcol = mod(col, G)
    srow, scol = solver_of(a)
    srel = srow - G * a
    is_s = (row == srow) & (col == scol)
    ours = G * mod(a, 2)
    near = mod(a + 1, 2)
    is_join = (col == JOIN) & (a > 0)
    lends = (half == near) & (a > 0)
    is_source = (row == SOURCE[0]) & (col == SOURCE[1])
    is_relay = (row == RELAY[0]) & (col == RELAY[1])

    width = G * TILE
    loads = [
        pltpu.make_async_copy(bt_hbm.at[0], bt_v, lsem.at[0]),
        pltpu.make_async_copy(cx_hbm.at[0], cx_v, lsem.at[1]),
        pltpu.make_async_copy(blocks_hbm, blocks_s, lsem.at[2]),
        pltpu.make_async_copy(rank_hbm.at[0, 0], rank_s, lsem.at[3]),
        pltpu.make_async_copy(u_hbm.at[0, 0, 0], u_v, lsem.at[4]),
        pltpu.make_async_copy(v_hbm.at[0, 0, 0], v_v, lsem.at[5]),
        pltpu.make_async_copy(
            rhs_hbm.at[:, pl.ds(pl.multiple_of(width * a, width), width)], rhs_v, lsem.at[6]
        ),
        pltpu.make_async_copy(diag_hbm.at[pl.ds(G * a, G)], d_v, lsem.at[7]),
        pltpu.make_async_copy(ci_hbm.at[0], ci_v, lsem.at[8]),
    ]
    for load in loads:
        load.start()

    def remote(src, dst, send, recv, r, c):
        return pltpu.make_async_remote_copy(
            src_ref=src, dst_ref=dst, send_sem=send, recv_sem=recv,
            device_id=(r, c), device_id_type=MESH,
        )

    bar = pltpu.get_barrier_semaphore()

    def signal(r, c):
        pl.semaphore_signal(bar, inc=1, device_id=(r, c), device_id_type=MESH)

    for k in range(1, N_ROW):
        signal(mod(row + k, N_ROW), col)

    @pl.when(jnp.logical_not(is_s))
    def _():
        signal(srow, scol)

    for b in range(2):
        @pl.when(half + 2 * b < a)
        def _():
            signal(*solver_of(half + 2 * b))

    @pl.when(is_s)
    def _():
        me = ii * N_COL + col
        for k in range(1, G * N_COL):
            other = mod(me + k, G * N_COL)
            signal(G * a + div(other, N_COL), mod(other, N_COL))
        for da in range(1, NG):
            @pl.when(a + da < NG)
            def _():
                for n in range(G * G):
                    signal(G * (a + da) + n // G, ours + n % G)

    @pl.when(lends & (col != JOIN))
    def _():
        signal(row, jnp.int32(JOIN))

    @pl.when(is_join)
    def _():
        for jj in range(G):
            c = G * near + jj
            pl.when(c != JOIN)(lambda: signal(row, c))
        signal(*solver_of(a - 1))

    @pl.when(is_s & (a + 1 < NG))
    def _():
        for i2 in range(G):
            signal(G * (a + 1) + i2, jnp.int32(JOIN))

    @pl.when(is_source)
    def _():
        signal(jnp.int32(RELAY[0]), jnp.int32(RELAY[1]))

    @pl.when(is_relay)
    def _():
        signal(jnp.int32(SOURCE[0]), jnp.int32(SOURCE[1]))

    greeted = (
        N_ROW - 1
        + jnp.where(is_source | is_relay, 1, 0)
        + jnp.where(lends & (col != JOIN), 1, 0)
        + jnp.where(is_join, G + 1 - jnp.where(lends, 1, 0), 0)
        + jnp.where(is_s & (a + 1 < NG), G, 0)
        + jnp.where(is_s, G * N_COL - 1 + G * G * (NG - 1 - a), 1)
        + jnp.where(half < a, 1, 0)
        + jnp.where(half + 2 < a, 1, 0)
    )

    lane = lax.broadcasted_iota(jnp.int32, (RHS, RMAX), 1)
    loads[3].wait()
    live = [lane < rank_s[0, b] for b in range(2)]

    with jax.named_scope("up"):
        loads[1].wait()
        loads[2].wait()
        loads[0].wait()
        up = nn(cx_v[...], bt_v[...])
        pieces = [up[:, m * BLK:(m + 1) * BLK] for m in range(BB)]
        ids = [jnp.full((RHS, BLK), blocks_s[0, m], jnp.int32) for m in range(BB)]

        @pl.loop(0, NT)
        def _(r):
            for q in range(QB):
                block = jnp.zeros((RHS, BLK), F32)
                for m in range(BB):
                    block = block + jnp.where(ids[m] == r * (QB) + q, pieces[m], 0.0)
                childp[r, :, q * BLK:(q + 1) * BLK] = block

    loads[4].wait()
    loads[5].wait()
    slot = div(a, 2)
    owner = (half == mod(a, 2)) & (jcol < ii)
    t_idx = div(ii * (ii - 1), 2) + jcol
    own_tile = jnp.where(owner & is_s, t_idx, -1)
    own_lent = lends & is_join
    from_slot = jnp.where(lends, div(a + 1, 2) - 1, slot)

    @pl.when(owner | lends)
    def _():
        us[...] = u_v[from_slot].astype(F32)
        wide = lax.broadcasted_iota(jnp.int32, (TILE, RMAX), 1)
        vs[...] = jnp.where(wide < rank_s[0, from_slot], v_v[from_slot].astype(F32), 0.0)

    @pl.when(owner & is_s)
    def _():
        urx[t_idx] = us[...]
        vrx[t_idx] = vs[...]

    @pl.when(own_lent)
    def _():
        ujoin[jcol] = us[...]
        vjoin[jcol] = vs[...]

    with jax.named_scope("bar"):
        pl.semaphore_wait(bar, greeted)

    def peer_row(k, sign=1):
        dy, dz = FAR_FIRST[k - 1]
        return G * mod(a + G + sign * dy, NG) + mod(ii + G + sign * dz, G)

    def child_copy(k):
        peer = peer_row(k)
        return remote(childp.at[peer], childrx.at[k - 1], csend.at[0], crecv.at[0], peer, col)

    def all_children():
        every = pl.ds(0, N_ROW - 1)
        return remote(
            childp.at[every], childrx.at[every], csend.at[0], crecv.at[0], srow, scol
        )

    def v_copy():
        return remote(vs, vrx.at[t_idx], tsend.at[0], trecv.at[0, t_idx], srow, scol)

    def u_copy():
        return remote(us, urx.at[t_idx], tsend.at[1], trecv.at[1, t_idx], srow, scol)

    def relay_in():
        return remote(
            us, urelay, tsend.at[1], rrecv.at[0], jnp.int32(RELAY[0]), jnp.int32(RELAY[1])
        )

    def relay_out():
        t = pair(*SOURCE)
        return remote(urelay, urx.at[t], rsend.at[0], trecv.at[1, t], srow, scol)

    def lend_copy(n, src, dst):
        return remote(
            src, dst.at[jcol], tsend.at[n], jtile.at[n, jcol], row, jnp.int32(JOIN)
        )

    lends_out = lends & (col != JOIN)
    sends_tile = owner & jnp.logical_not(is_s)
    sends_u = sends_tile & jnp.logical_not(is_source)
    pl.when(is_source)(lambda: relay_in().start())
    for k in range(1, N_ROW):
        child_copy(k).start()
    pl.when(sends_tile)(lambda: v_copy().start())
    pl.when(sends_u)(lambda: u_copy().start())

    @pl.when(lends_out)
    def _():
        lend_copy(0, vs, vjoin).start()
        lend_copy(1, us, ujoin).start()

    with jax.named_scope("child_wait"):
        all_children().wait_recv()
        total = childp[row]
        for k in range(N_ROW - 1):
            total = total + childrx[k]
        rowmsg[...] = total

    tiles = [(i, j) for i in range(G) for j in range(i)]

    def turn():
        with jax.named_scope("turn"):
            for jj in range(G):
                dt[jj] = d_v[jj].T
            for i, j in tiles:
                t = pair(i, j)
                utin[t] = urx[t].T.astype(BF16)
                wb[t] = nn(vrx[t].T.astype(BF16), dt[j]).astype(BF16)

    loads[7].wait()

    @pl.when(is_s)
    def _():
        with jax.named_scope("tiles_wait"):
            for i, j in ((3, 1), (3, 0), (3, 2), (1, 0), (2, 0), (2, 1)):
                t = pair(i, j)

                @pl.when(own_tile != t)
                def _():
                    with jax.named_scope(f"tv{i}{j}"):
                        remote(vs, vrx.at[t], tsend.at[0], trecv.at[0, t], srow, scol).wait_recv()
                    with jax.named_scope(f"tu{i}{j}"):
                        remote(us, urx.at[t], tsend.at[1], trecv.at[1, t], srow, scol).wait_recv()

                vbf[t] = vrx[t].astype(BF16)
                wf[t] = nn(urx[t].astype(BF16), d_v[i]).astype(BF16)
        pl.when(a == NG - 1)(turn)

    def is_older(b):
        return half + 2 * b + 1 < a

    with jax.named_scope("turn2"):
        for b in range(2):
            @pl.when(is_older(b))
            def _():
                ut[b] = u_v[b].T
                vt[b] = v_v[b].T

        @pl.when(is_join)
        def _():
            for jj in range(G):
                @pl.when(G * near + jj != JOIN)
                def _():
                    remote(
                        vs, vjoin.at[jj], tsend.at[0], jtile.at[0, jj], row, jnp.int32(0)
                    ).wait_recv()
                    remote(
                        us, ujoin.at[jj], tsend.at[1], jtile.at[1, jj], row, jnp.int32(0)
                    ).wait_recv()

                vj[jj] = vjoin[jj].astype(BF16)
                uj[jj] = ujoin[jj].astype(BF16)
                vjt[jj] = vjoin[jj].T.astype(BF16)
                ujt[jj] = ujoin[jj].T.astype(BF16)

    with jax.named_scope("fwd_row"):
        for b in range(2):
            @pl.when(is_older(b))
            def _():
                remote(xs.at[0], xrx.at[b], xsend.at[0], xrecv.at[b], srow, scol).wait_recv()
                p = nn(xrx[b].astype(BF16), v_v[b])
                p = jnp.where(live[b], p, 0.0).astype(BF16)
                rowmsg[...] += nn(p, u_v[b])

        @pl.when(is_join)
        def _():
            for jj in range(G):
                remote(
                    xs.at[0], xjoin.at[jj], xsend.at[0], xjrecv.at[jj], srow, scol
                ).wait_recv()
                p = nn(xjoin[jj].astype(BF16), vj[jj]).astype(BF16)
                rowmsg[...] += nn(p, uj[jj])

    def row_copy():
        return remote(
            rowmsg, srx.at[ii, col], msend.at[0], srecv.at[ii], srow, scol
        )

    @pl.when(is_s)
    def _():
        srx[ii, col] = rowmsg[...]

    @pl.when(jnp.logical_not(is_s))
    def _():
        row_copy().start()

    @pl.when(is_relay)
    def _():
        relay_in().wait_recv()
        relay_out().start()

    loads[6].wait()

    def x_copy(jj, da, i2):
        if da == 1:
            return remote(
                xs.at[jj], xjoin.at[jj], xsend.at[0], xjrecv.at[jj],
                G * (a + 1) + i2, jnp.int32(JOIN),
            )
        return remote(
            xs.at[jj], xrx.at[slot], xsend.at[da - 1], xrecv.at[slot],
            G * (a + da) + i2, ours + jj,
        )

    @pl.when(is_s)
    def _():
        def wait_row(jj, count):
            slots = srx.at[jj, pl.ds(0, count)]
            remote(slots, slots, msend.at[0], srecv.at[jj], srow, scol).wait_recv()

        def wait_all(jj):
            with jax.named_scope(f"s_fwd_wait{jj}"):
                pl.when(srel != jj)(lambda: wait_row(jj, N_COL))
                pl.when(srel == jj)(lambda: wait_row(jj, N_COL - 1))

        def base(jj):
            parts = [srx[jj, c] for c in range(N_COL)]
            while len(parts) > 1:
                parts = [parts[n] + parts[n + 1] for n in range(0, len(parts), 2)]
            right = rhs_v[:, jj * TILE:(jj + 1) * TILE].astype(F32) - parts[0]
            return folded(nn(two_halves(right), d_v[jj]))

        x = [None] * G

        def publish(jj):
            xs[jj] = x[jj]

            @pl.when(a + 1 < NG)
            def _():
                for i2 in range(G):
                    x_copy(jj, 1, i2).start()

        wait_all(0)
        x[0] = base(0)
        publish(0)
        for jj in range(1, G):
            wait_all(jj)
            done = x[jj - 1].astype(BF16)
            for mm in range(jj, G):
                t = pair(mm, jj - 1)
                part = nn(nn(done, vbf[t]).astype(BF16), wf[t])
                x[mm] = part if x[mm] is None else x[mm] + part
            x[jj] = base(jj) - x[jj]
            publish(jj)
        for da in range(2, NG):
            @pl.when(a + da < NG)
            def _():
                for i2 in range(G):
                    for jj in range(G):
                        x_copy(jj, da, i2).start()
        pl.when(a < NG - 1)(turn)

    all_children().wait_send()
    @pl.when(lends_out)
    def _():
        lend_copy(0, vs, vjoin).wait_send()
        lend_copy(1, us, ujoin).wait_send()

    pl.when(sends_tile)(lambda: v_copy().wait_send())
    pl.when(sends_u)(lambda: u_copy().wait_send())
    pl.when(is_source)(lambda: relay_in().wait_send())
    pl.when(is_relay)(lambda: relay_out().wait_send())
    pl.when(jnp.logical_not(is_s))(lambda: row_copy().wait_send())

    def z_tile(i):
        return zfull.at[pl.ds(QB * i, QB)]

    def z_copy(jj, k):
        c = mod(JOIN + k, N_COL)
        return c, remote(
            zs.at[jj], z_tile(G * a + jj), zsend.at[jj], zrecv.at[0], G * a + jj, c
        )

    may_be_own = {(SOLVER_COL[g] - JOIN) % N_COL for g in range(NG)}

    @pl.when(is_s)
    def _():
        def wait_da(jj, da):
            slots = brx.at[jj, pl.ds((da - 1) * G, G)]
            remote(slots, slots, bsend.at[0], brecv.at[jj, da - 1], srow, scol).wait_recv()

        def take(jj, da):
            n = (da - 1) * G
            tacc[jj] -= (brx[jj, n] + brx[jj, n + 1]) + (brx[jj, n + 2] + brx[jj, n + 3])

        def collect(rows, das):
            for da in das:
                @pl.when(a + da < NG)
                def _():
                    for jj in rows:
                        wait_da(jj, da)
                    for jj in rows:
                        take(jj, da)

        def base(jj):
            return folded(nn(two_halves(tacc[jj]), dt[jj]))

        z = [None] * G

        def publish(jj):
            for q in range(QB):
                part = z[jj][:, q * BLK:(q + 1) * BLK]
                zs[jj, q] = part
                zfull[QB * (G * a + jj) + q] = part
            for k in range(N_COL):
                c, copy = z_copy(jj, k)
                if k in may_be_own:
                    pl.when((srel != jj) | (c != col))(copy.start)
                else:
                    copy.start()

        tacc[...] = xs[...]
        with jax.named_scope("s_bwd_old"):
            collect(range(G), range(NG - 1, 1, -1))
        last = G - 1
        with jax.named_scope("s_bwd_wait3"):
            collect((last,), (1,))
        z[last] = base(last)
        publish(last)
        for jj in range(last - 1, -1, -1):
            with jax.named_scope(f"s_bwd_wait{jj}"):
                collect((jj,), (1,))
            done = z[jj + 1].astype(BF16)
            for mm in range(jj, -1, -1):
                t = pair(jj + 1, mm)
                part = nn(nn(done, utin[t]).astype(BF16), wb[t])
                z[mm] = part if z[mm] is None else z[mm] + part
            z[jj] = base(jj) - z[jj]
            publish(jj)

    @pl.when(jnp.logical_not(is_s))
    def _():
        with jax.named_scope("z_wait"):
            remote(zs.at[0], z_tile(row), zsend.at[0], zrecv.at[0], srow, scol).wait_recv()

    def back_copy(b):
        g = half + 2 * b
        n = (a - g - 1) * G + ii
        return remote(
            bmsg.at[b], brx.at[jcol, n], bsend.at[b], brecv.at[jcol, a - g - 1], *solver_of(g)
        )

    def join_copy(jj):
        return remote(
            bjoin.at[jj], brx.at[jj, ii], bjsend.at[0], brecv.at[jj, 0], *solver_of(a - 1)
        )

    @pl.when(is_join)
    def _():
        zb = jnp.concatenate([zfull[QB * row + q] for q in range(QB)], axis=1).astype(BF16)
        for jj in reversed(range(G)):
            bjoin[jj] = nn(nn(zb, ujt[jj]).astype(BF16), vjt[jj])
            join_copy(jj).start()

    mine = jnp.concatenate([zfull[QB * row + q] for q in range(QB)], axis=1)
    for b in reversed(range(2)):
        @pl.when(is_older(b))
        def _():
            q = nn(mine.astype(BF16), ut[b])
            q = jnp.where(live[b], q, 0.0).astype(BF16)
            bmsg[b] = nn(q, vt[b])
            back_copy(b).start()

    def gather_copy(k):
        peer = peer_row(k)
        return remote(z_tile(row), z_tile(row), gsend.at[0], grecv.at[0], peer, col)

    def all_gathered():
        every = zfull.at[pl.ds(0, QB * (N_ROW - 1))]
        return remote(every, every, gsend.at[0], grecv.at[0], srow, scol)

    for k in range(1, N_ROW):
        gather_copy(k).start()

    wide = zfull[QB * row + div(col, 2)]
    root_out[...] = jnp.where(mod(col, 2) == 0, wide[:, :HALF], wide[:, HALF:])

    for b in range(2):
        @pl.when(is_older(b))
        def _():
            back_copy(b).wait_send()

    @pl.when(is_join)
    def _():
        remote(bjoin, bjoin, bjsend.at[0], brecv.at[0, 0], srow, scol).wait_send()

    @pl.when(is_s)
    def _():
        for da in range(1, NG):
            @pl.when(a + da < NG)
            def _():
                slots = brx.at[:, pl.ds(0, G)]
                remote(slots, slots, xsend.at[da - 1], xrecv.at[0], srow, scol).wait_send()
        for jj in range(G):
            def wait_z(count):
                slots = srx.at[jj, pl.ds(0, count)]
                remote(slots, slots, zsend.at[jj], zrecv.at[0], srow, scol).wait_send()

            pl.when(srel != jj)(lambda: wait_z(N_COL))
            pl.when(srel == jj)(lambda: wait_z(N_COL - 1))

    with jax.named_scope("gather_wait"):
        all_gathered().wait_recv()

    with jax.named_scope("final"):
        loads[8].wait()
        parts = [zfull[blocks_s[0, m]] for m in range(BB)]
        gathered = jnp.concatenate(parts, axis=1).astype(BF16)
        returned = nt(gathered, bt_v[...])
        child_out[0] = cx_v[...].astype(F32) - folded(nn(two_halves(returned), ci_v[...]))

    all_gathered().wait_send()


def per_device(
    root_rhs, diag_inv, tile_u, tile_v, tile_rank, child_x, border_t, child_inv, child_blocks
):
    vmem = pl.BlockSpec(memory_space=pltpu.VMEM)
    hbm = pl.BlockSpec(memory_space=pltpu.HBM)
    dma = pltpu.SemaphoreType.DMA
    pairs = G * (G - 1) // 2
    wide = (RHS, TILE)
    return pl.pallas_call(
        kernel,
        out_shape=(
            jax.ShapeDtypeStruct((RHS, HALF), F32),
            jax.ShapeDtypeStruct((1, RHS, TILE), F32),
        ),
        in_specs=[hbm] * 9,
        out_specs=(vmem, vmem),
        scratch_shapes=[
            pltpu.VMEM((RHS, G * TILE), BF16),
            pltpu.VMEM(wide, BF16),
            pltpu.SMEM((1, BB), jnp.int32),
            pltpu.SMEM((1, 2), jnp.int32),
            pltpu.VMEM((RMAX, TILE), F32),
            pltpu.VMEM((G, TILE, TILE), BF16),
            pltpu.VMEM((2, TILE, RMAX), BF16),
            pltpu.VMEM((2, RMAX, TILE), BF16),
            pltpu.VMEM((pairs, TILE, RMAX), BF16),
            pltpu.VMEM((G, TILE, RMAX), F32),
            pltpu.VMEM((G, RMAX, TILE), F32),
            pltpu.VMEM((G, TILE, RMAX), BF16),
            pltpu.VMEM((G, RMAX, TILE), BF16),
            pltpu.VMEM((G, RMAX, TILE), BF16),
            pltpu.VMEM((G, TILE, RMAX), BF16),
            pltpu.VMEM((G, *wide), F32),
            pltpu.VMEM((G, *wide), F32),
            pltpu.VMEM((TILE, BB * BLK), BF16),
            pltpu.VMEM((TILE, TILE), BF16),
            pltpu.VMEM((2, RMAX, TILE), BF16),
            pltpu.VMEM((2, TILE, RMAX), BF16),
            pltpu.VMEM((G, TILE, TILE), BF16),
            pltpu.VMEM((RMAX, TILE), F32),
            pltpu.VMEM((TILE, RMAX), F32),
            pltpu.VMEM((pairs, RMAX, TILE), F32),
            pltpu.VMEM((pairs, TILE, RMAX), F32),
            pltpu.VMEM((pairs, RMAX, TILE), BF16),
            pltpu.VMEM((pairs, RMAX, TILE), BF16),
            pltpu.VMEM((pairs, TILE, RMAX), BF16),
            pltpu.VMEM((NT, *wide), F32),
            pltpu.VMEM((N_ROW, *wide), F32),
            pltpu.VMEM((2, *wide), F32),
            pltpu.VMEM(wide, F32),
            pltpu.VMEM((G, N_COL, *wide), F32),
            pltpu.VMEM((G, *wide), F32),
            pltpu.VMEM((NT * QB, RHS, BLK), F32),
            pltpu.VMEM((G, QB, RHS, BLK), F32),
            pltpu.VMEM((2, *wide), F32),
            pltpu.VMEM((G, (NG - 1) * G, *wide), F32),
            pltpu.VMEM((G, *wide), F32),
            dma((9,)),
            dma((1,)),
            dma((1,)),
            dma((2,)),
            dma((2, pairs)),
            dma((1,)),
            dma((G,)),
            dma((NG - 1,)),
            dma((2,)),
            dma((G,)),
            dma((1,)),
            dma((2,)),
            dma((G, NG - 1)),
            dma((1,)),
            dma((1,)),
            dma((1,)),
            dma((1,)),
            dma((2, G)),
            dma((G,)),
            dma((1,)),
        ],
        compiler_params=pltpu.CompilerParams(
            collective_id=0, has_side_effects=True, vmem_limit_bytes=48_000_000
        ),
    )(
        *(
            pltpu.with_memory_space_constraint(array, pltpu.HBM)
            for array in (
                root_rhs, child_x, child_blocks, tile_rank, diag_inv,
                tile_u, tile_v, border_t, child_inv,
            )
        )
    )


def solution(mesh):
    both = ("row", "col")
    tiles = P("row", "col", None, None, None, None)
    in_specs = (
        P(),
        P(),
        tiles,
        tiles,
        P("row", "col", None, None),
        P(both, None, None),
        P(both, None, None),
        P(both, None, None),
        P(both, None),
    )
    out_specs = (P(None, both), P(both, None, None))
    return jax.shard_map(
        per_device, mesh=mesh, in_specs=in_specs, out_specs=out_specs, check_vma=False
    )
```

```python
import jax
import jax.numpy as jnp
from jax import lax
from jax.experimental import pallas as pl
from jax.experimental.pallas import tpu as pltpu
from jax.sharding import PartitionSpec as P

MESH = pl.DeviceIdType.MESH
F32 = jnp.float32
BF16 = jnp.bfloat16
NT = 16
TILE = 512
RHS = 8
RMAX = 128
BLK = 128
BB = 8
N_ROW = 16
N_COL = 8
G = 4
NG = NT // G
SOLVER_ROW = (3, 3, 0, 1)
SOLVER_COL = (1, 3, 3, 3)
JOIN = 3
FAR_FIRST = (
    (2, 2), (3, 2), (0, 2), (2, 3), (3, 3), (0, 1), (2, 1), (3, 1), (0, 3),
    (1, 2), (3, 0), (1, 3), (1, 1), (2, 0), (1, 0),
)
SOURCE = (2, 0)
RELAY = (3, 3)
VIA = ((10, 8, (0, 1)), (14, 13, (5,)))
HALF = TILE // N_COL
QB = TILE // BLK


def div(x, n):
    return lax.div(x, jnp.int32(n))


def mod(x, n):
    return lax.rem(x, jnp.int32(n))


def pick(table, group):
    if isinstance(group, int):
        return jnp.int32(table[group])
    value = jnp.int32(table[-1])
    for g in range(len(table) - 1):
        value = jnp.where(group == g, jnp.int32(table[g]), value)
    return value


def solver_of(group):
    return G * group + pick(SOLVER_ROW, group), pick(SOLVER_COL, group)


def pair(i, j):
    return i * (i - 1) // 2 + j


def nn(a, b):
    return lax.dot_general(a, b, (((1,), (0,)), ((), ())), preferred_element_type=F32)


def nt(a, b):
    return lax.dot_general(a, b, (((1,), (1,)), ((), ())), preferred_element_type=F32)


def two_halves(t):
    hi = t.astype(BF16).astype(F32)
    return jnp.concatenate([hi, t - hi], axis=0).astype(BF16)


def folded(r):
    return r[:RHS] + r[RHS:]


def kernel(
    rhs_hbm, cx_hbm, blocks_hbm, rank_hbm, diag_hbm, u_hbm, v_hbm, bt_hbm, ci_hbm,
    root_out, child_out,
    rhs_v, cx_v, blocks_s, rank_s, urelay, dt, ut, vt, utin,
    vjoin, ujoin, vj, uj, vjt, ujt, xjoin, bjoin,
    bt_v, ci_v, u_v, v_v, d_v, us, vs, urx, vrx, wf, wb, vbf,
    childp, childrx, xrx, rowmsg, srx, xs, zfull, zs, bmsg, brx, tacc,
    lsem, csend, crecv, tsend, trecv, msend, srecv, xsend, xrecv,
    zsend, zrecv, bsend, brecv, gsend, grecv, rsend, rrecv, jtile, xjrecv, bjsend, viarecv,
):
    row = lax.axis_index("row")
    col = lax.axis_index("col")
    a = div(row, G)
    ii = mod(row, G)
    half = div(col, G)
    jcol = mod(col, G)
    srow, scol = solver_of(a)
    srel = srow - G * a
    is_s = (row == srow) & (col == scol)
    ours = G * mod(a, 2)
    near = mod(a + 1, 2)
    is_join = (col == JOIN) & (a > 0)
    lends = (half == near) & (a > 0)
    via_source = row < 0
    is_via = row < 0
    via_row = jnp.int32(VIA[-1][1])
    for start, stop, columns in VIA:
        for c in columns:
            via_source = via_source | ((row == start) & (col == c))
            is_via = is_via | ((row == stop) & (col == c))
        via_row = jnp.where(row == start, jnp.int32(stop), via_row)
    is_source = (row == SOURCE[0]) & (col == SOURCE[1])
    is_relay = (row == RELAY[0]) & (col == RELAY[1])

    width = G * TILE
    loads = [
        pltpu.make_async_copy(bt_hbm.at[0], bt_v, lsem.at[0]),
        pltpu.make_async_copy(cx_hbm.at[0], cx_v, lsem.at[1]),
        pltpu.make_async_copy(blocks_hbm, blocks_s, lsem.at[2]),
        pltpu.make_async_copy(rank_hbm.at[0, 0], rank_s, lsem.at[3]),
        pltpu.make_async_copy(u_hbm.at[0, 0, 0], u_v, lsem.at[4]),
        pltpu.make_async_copy(v_hbm.at[0, 0, 0], v_v, lsem.at[5]),
        pltpu.make_async_copy(
            rhs_hbm.at[:, pl.ds(pl.multiple_of(width * a, width), width)], rhs_v, lsem.at[6]
        ),
        pltpu.make_async_copy(diag_hbm.at[pl.ds(G * a, G)], d_v, lsem.at[7]),
        pltpu.make_async_copy(ci_hbm.at[0], ci_v, lsem.at[8]),
    ]
    for load in loads:
        load.start()

    def remote(src, dst, send, recv, r, c):
        return pltpu.make_async_remote_copy(
            src_ref=src, dst_ref=dst, send_sem=send, recv_sem=recv,
            device_id=(r, c), device_id_type=MESH,
        )

    bar = pltpu.get_barrier_semaphore()

    def signal(r, c):
        pl.semaphore_signal(bar, inc=1, device_id=(r, c), device_id_type=MESH)

    for k in range(1, N_ROW):
        signal(mod(row + k, N_ROW), col)

    @pl.when(jnp.logical_not(is_s))
    def _():
        signal(srow, scol)

    for b in range(2):
        @pl.when(half + 2 * b < a)
        def _():
            signal(*solver_of(half + 2 * b))

    @pl.when(is_s)
    def _():
        me = ii * N_COL + col
        for k in range(1, G * N_COL):
            other = mod(me + k, G * N_COL)
            signal(G * a + div(other, N_COL), mod(other, N_COL))
        for da in range(1, NG):
            @pl.when(a + da < NG)
            def _():
                for n in range(G * G):
                    signal(G * (a + da) + n // G, ours + n % G)

    @pl.when(lends & (col != JOIN))
    def _():
        signal(row, jnp.int32(JOIN))

    @pl.when(is_join)
    def _():
        for jj in range(G):
            c = G * near + jj
            pl.when(c != JOIN)(lambda: signal(row, c))
        signal(*solver_of(a - 1))

    @pl.when(is_s & (a + 1 < NG))
    def _():
        for i2 in range(G):
            signal(G * (a + 1) + i2, jnp.int32(JOIN))

    @pl.when(is_source)
    def _():
        signal(jnp.int32(RELAY[0]), jnp.int32(RELAY[1]))

    @pl.when(is_relay)
    def _():
        signal(jnp.int32(SOURCE[0]), jnp.int32(SOURCE[1]))

    greeted = (
        N_ROW - 1
        + jnp.where(is_source | is_relay, 1, 0)
        + jnp.where(lends & (col != JOIN), 1, 0)
        + jnp.where(is_join, G + 1 - jnp.where(lends, 1, 0), 0)
        + jnp.where(is_s & (a + 1 < NG), G, 0)
        + jnp.where(is_s, G * N_COL - 1 + G * G * (NG - 1 - a), 1)
        + jnp.where(half < a, 1, 0)
        + jnp.where(half + 2 < a, 1, 0)
    )

    lane = lax.broadcasted_iota(jnp.int32, (RHS, RMAX), 1)
    loads[3].wait()
    live = [lane < rank_s[0, b] for b in range(2)]

    with jax.named_scope("up"):
        loads[1].wait()
        loads[2].wait()
        loads[0].wait()
        up = nn(cx_v[...], bt_v[...])
        pieces = [up[:, m * BLK:(m + 1) * BLK] for m in range(BB)]
        ids = [jnp.full((RHS, BLK), blocks_s[0, m], jnp.int32) for m in range(BB)]

        @pl.loop(0, NT)
        def _(r):
            for q in range(QB):
                block = jnp.zeros((RHS, BLK), F32)
                for m in range(BB):
                    block = block + jnp.where(ids[m] == r * (QB) + q, pieces[m], 0.0)
                childp[r, :, q * BLK:(q + 1) * BLK] = block

    loads[4].wait()
    loads[5].wait()
    slot = div(a, 2)
    owner = (half == mod(a, 2)) & (jcol < ii)
    t_idx = div(ii * (ii - 1), 2) + jcol
    own_tile = jnp.where(owner & is_s, t_idx, -1)
    own_lent = lends & is_join
    from_slot = jnp.where(lends, div(a + 1, 2) - 1, slot)

    @pl.when(owner | lends)
    def _():
        us[...] = u_v[from_slot].astype(F32)
        wide = lax.broadcasted_iota(jnp.int32, (TILE, RMAX), 1)
        vs[...] = jnp.where(wide < rank_s[0, from_slot], v_v[from_slot].astype(F32), 0.0)

    @pl.when(owner & is_s)
    def _():
        urx[t_idx] = us[...]
        vrx[t_idx] = vs[...]

    @pl.when(own_lent)
    def _():
        ujoin[jcol] = us[...]
        vjoin[jcol] = vs[...]

    with jax.named_scope("bar"):
        pl.semaphore_wait(bar, greeted)

    def peer_row(k, sign=1):
        dy, dz = FAR_FIRST[k - 1]
        return G * mod(a + G + sign * dy, NG) + mod(ii + G + sign * dz, G)

    def child_copy(k):
        peer = peer_row(k)
        return remote(childp.at[peer], childrx.at[k - 1], csend.at[0], crecv.at[0], peer, col)

    def all_children():
        every = pl.ds(0, N_ROW - 1)
        return remote(
            childp.at[every], childrx.at[every], csend.at[0], crecv.at[0], srow, scol
        )

    def v_copy():
        return remote(vs, vrx.at[t_idx], tsend.at[0], trecv.at[0, t_idx], srow, scol)

    def u_copy():
        return remote(us, urx.at[t_idx], tsend.at[1], trecv.at[1, t_idx], srow, scol)

    def relay_in():
        return remote(
            us, urelay, tsend.at[1], rrecv.at[0], jnp.int32(RELAY[0]), jnp.int32(RELAY[1])
        )

    def relay_out():
        t = pair(*SOURCE)
        return remote(urelay, urx.at[t], rsend.at[0], trecv.at[1, t], srow, scol)

    def lend_copy(n, src, dst):
        return remote(
            src, dst.at[jcol], tsend.at[n], jtile.at[n, jcol], row, jnp.int32(JOIN)
        )

    lends_out = lends & (col != JOIN)
    def via_in(n, ref):
        return remote(
            ref, ref, tsend.at[n], viarecv.at[n], via_row, col
        )

    def via_out(n, ref, dst):
        t = pair(2, 0) + jcol
        return remote(ref, dst.at[t], tsend.at[n], trecv.at[n, t], srow, scol)

    sends_tile = owner & jnp.logical_not(is_s | via_source)
    sends_u = sends_tile & jnp.logical_not(is_source)
    pl.when(is_source)(lambda: relay_in().start())
    for k in range(1, N_ROW):
        child_copy(k).start()
    pl.when(sends_tile)(lambda: v_copy().start())
    pl.when(sends_u)(lambda: u_copy().start())

    @pl.when(via_source)
    def _():
        via_in(0, vs).start()
        via_in(1, us).start()

    @pl.when(lends_out)
    def _():
        lend_copy(0, vs, vjoin).start()
        lend_copy(1, us, ujoin).start()

    with jax.named_scope("child_wait"):
        all_children().wait_recv()
        total = childp[row]
        for k in range(N_ROW - 1):
            total = total + childrx[k]
        rowmsg[...] = total

    @pl.when(is_via)
    def _():
        via_in(0, vs).wait_recv()
        via_out(0, vs, vrx).start()
        via_in(1, us).wait_recv()
        via_out(1, us, urx).start()

    tiles = [(i, j) for i in range(G) for j in range(i)]

    def turn():
        with jax.named_scope("turn"):
            for jj in range(G):
                dt[jj] = d_v[jj].T
            for i, j in tiles:
                t = pair(i, j)
                utin[t] = urx[t].T.astype(BF16)
                wb[t] = nn(vrx[t].T.astype(BF16), dt[j]).astype(BF16)

    loads[7].wait()

    @pl.when(is_s)
    def _():
        with jax.named_scope("tiles_wait"):
            for i, j in ((3, 1), (3, 0), (3, 2), (1, 0), (2, 0), (2, 1)):
                t = pair(i, j)

                @pl.when(own_tile != t)
                def _():
                    with jax.named_scope(f"tv{i}{j}"):
                        remote(vs, vrx.at[t], tsend.at[0], trecv.at[0, t], srow, scol).wait_recv()
                    with jax.named_scope(f"tu{i}{j}"):
                        remote(us, urx.at[t], tsend.at[1], trecv.at[1, t], srow, scol).wait_recv()

                vbf[t] = vrx[t].astype(BF16)
                wf[t] = nn(urx[t].astype(BF16), d_v[i]).astype(BF16)
        pl.when(a == NG - 1)(turn)

    def is_older(b):
        return half + 2 * b + 1 < a

    with jax.named_scope("turn2"):
        for b in range(2):
            @pl.when(is_older(b))
            def _():
                ut[b] = u_v[b].T
                vt[b] = v_v[b].T

        @pl.when(is_join)
        def _():
            for jj in range(G):
                @pl.when(G * near + jj != JOIN)
                def _():
                    remote(
                        vs, vjoin.at[jj], tsend.at[0], jtile.at[0, jj], row, jnp.int32(0)
                    ).wait_recv()
                    remote(
                        us, ujoin.at[jj], tsend.at[1], jtile.at[1, jj], row, jnp.int32(0)
                    ).wait_recv()

                vj[jj] = vjoin[jj].astype(BF16)
                uj[jj] = ujoin[jj].astype(BF16)
                vjt[jj] = vjoin[jj].T.astype(BF16)
                ujt[jj] = ujoin[jj].T.astype(BF16)

    with jax.named_scope("fwd_row"):
        for b in range(2):
            @pl.when(is_older(b))
            def _():
                remote(xs.at[0], xrx.at[b], xsend.at[0], xrecv.at[b], srow, scol).wait_recv()
                p = nn(xrx[b].astype(BF16), v_v[b])
                p = jnp.where(live[b], p, 0.0).astype(BF16)
                rowmsg[...] += nn(p, u_v[b])

        @pl.when(is_join)
        def _():
            for jj in range(G):
                remote(
                    xs.at[0], xjoin.at[jj], xsend.at[0], xjrecv.at[jj], srow, scol
                ).wait_recv()
                p = nn(xjoin[jj].astype(BF16), vj[jj]).astype(BF16)
                rowmsg[...] += nn(p, uj[jj])

    def row_copy():
        return remote(
            rowmsg, srx.at[ii, col], msend.at[0], srecv.at[ii], srow, scol
        )

    @pl.when(is_s)
    def _():
        srx[ii, col] = rowmsg[...]

    @pl.when(jnp.logical_not(is_s))
    def _():
        row_copy().start()

    @pl.when(is_relay)
    def _():
        relay_in().wait_recv()
        relay_out().start()

    loads[6].wait()

    def x_copy(jj, da, i2):
        if da == 1:
            return remote(
                xs.at[jj], xjoin.at[jj], xsend.at[0], xjrecv.at[jj],
                G * (a + 1) + i2, jnp.int32(JOIN),
            )
        return remote(
            xs.at[jj], xrx.at[slot], xsend.at[da - 1], xrecv.at[slot],
            G * (a + da) + i2, ours + jj,
        )

    @pl.when(is_s)
    def _():
        def wait_row(jj, count):
            slots = srx.at[jj, pl.ds(0, count)]
            remote(slots, slots, msend.at[0], srecv.at[jj], srow, scol).wait_recv()

        def wait_all(jj):
            with jax.named_scope(f"s_fwd_wait{jj}"):
                pl.when(srel != jj)(lambda: wait_row(jj, N_COL))
                pl.when(srel == jj)(lambda: wait_row(jj, N_COL - 1))

        def base(jj):
            parts = [srx[jj, c] for c in range(N_COL)]
            while len(parts) > 1:
                parts = [parts[n] + parts[n + 1] for n in range(0, len(parts), 2)]
            right = rhs_v[:, jj * TILE:(jj + 1) * TILE].astype(F32) - parts[0]
            return folded(nn(two_halves(right), d_v[jj]))

        x = [None] * G

        def publish(jj):
            xs[jj] = x[jj]

            @pl.when(a + 1 < NG)
            def _():
                for i2 in range(G):
                    x_copy(jj, 1, i2).start()

        wait_all(0)
        x[0] = base(0)
        publish(0)
        for jj in range(1, G):
            wait_all(jj)
            done = x[jj - 1].astype(BF16)
            for mm in range(jj, G):
                t = pair(mm, jj - 1)
                part = nn(nn(done, vbf[t]).astype(BF16), wf[t])
                x[mm] = part if x[mm] is None else x[mm] + part
            x[jj] = base(jj) - x[jj]
            publish(jj)
        for da in range(2, NG):
            @pl.when(a + da < NG)
            def _():
                for i2 in range(G):
                    for jj in range(G):
                        x_copy(jj, da, i2).start()
        pl.when(a < NG - 1)(turn)

    all_children().wait_send()
    @pl.when(via_source)
    def _():
        via_in(0, vs).wait_send()
        via_in(1, us).wait_send()

    @pl.when(is_via)
    def _():
        via_out(0, vs, vrx).wait_send()
        via_out(1, us, urx).wait_send()

    @pl.when(lends_out)
    def _():
        lend_copy(0, vs, vjoin).wait_send()
        lend_copy(1, us, ujoin).wait_send()

    pl.when(sends_tile)(lambda: v_copy().wait_send())
    pl.when(sends_u)(lambda: u_copy().wait_send())
    pl.when(is_source)(lambda: relay_in().wait_send())
    pl.when(is_relay)(lambda: relay_out().wait_send())
    pl.when(jnp.logical_not(is_s))(lambda: row_copy().wait_send())

    def z_tile(i):
        return zfull.at[pl.ds(QB * i, QB)]

    def z_copy(jj, k):
        c = mod(JOIN + k, N_COL)
        return c, remote(
            zs.at[jj], z_tile(G * a + jj), zsend.at[jj], zrecv.at[0], G * a + jj, c
        )

    may_be_own = {(SOLVER_COL[g] - JOIN) % N_COL for g in range(NG)}

    @pl.when(is_s)
    def _():
        def wait_da(jj, da):
            slots = brx.at[jj, pl.ds((da - 1) * G, G)]
            remote(slots, slots, bsend.at[0], brecv.at[jj, da - 1], srow, scol).wait_recv()

        def take(jj, da):
            n = (da - 1) * G
            tacc[jj] -= (brx[jj, n] + brx[jj, n + 1]) + (brx[jj, n + 2] + brx[jj, n + 3])

        def collect(rows, das):
            for da in das:
                @pl.when(a + da < NG)
                def _():
                    for jj in rows:
                        wait_da(jj, da)
                    for jj in rows:
                        take(jj, da)

        def base(jj):
            return folded(nn(two_halves(tacc[jj]), dt[jj]))

        z = [None] * G

        def publish(jj):
            for q in range(QB):
                part = z[jj][:, q * BLK:(q + 1) * BLK]
                zs[jj, q] = part
                zfull[QB * (G * a + jj) + q] = part
            for k in range(N_COL):
                c, copy = z_copy(jj, k)
                if k in may_be_own:
                    pl.when((srel != jj) | (c != col))(copy.start)
                else:
                    copy.start()

        tacc[...] = xs[...]
        with jax.named_scope("s_bwd_old"):
            collect(range(G), range(NG - 1, 1, -1))
        last = G - 1
        with jax.named_scope("s_bwd_wait3"):
            collect((last,), (1,))
        z[last] = base(last)
        publish(last)
        for jj in range(last - 1, -1, -1):
            with jax.named_scope(f"s_bwd_wait{jj}"):
                collect((jj,), (1,))
            done = z[jj + 1].astype(BF16)
            for mm in range(jj, -1, -1):
                t = pair(jj + 1, mm)
                part = nn(nn(done, utin[t]).astype(BF16), wb[t])
                z[mm] = part if z[mm] is None else z[mm] + part
            z[jj] = base(jj) - z[jj]
            publish(jj)

    @pl.when(jnp.logical_not(is_s))
    def _():
        with jax.named_scope("z_wait"):
            remote(zs.at[0], z_tile(row), zsend.at[0], zrecv.at[0], srow, scol).wait_recv()

    def back_copy(b):
        g = half + 2 * b
        n = (a - g - 1) * G + ii
        return remote(
            bmsg.at[b], brx.at[jcol, n], bsend.at[b], brecv.at[jcol, a - g - 1], *solver_of(g)
        )

    def join_copy(jj):
        return remote(
            bjoin.at[jj], brx.at[jj, ii], bjsend.at[0], brecv.at[jj, 0], *solver_of(a - 1)
        )

    @pl.when(is_join)
    def _():
        zb = jnp.concatenate([zfull[QB * row + q] for q in range(QB)], axis=1).astype(BF16)
        for jj in reversed(range(G)):
            bjoin[jj] = nn(nn(zb, ujt[jj]).astype(BF16), vjt[jj])
            join_copy(jj).start()

    mine = jnp.concatenate([zfull[QB * row + q] for q in range(QB)], axis=1)
    for b in reversed(range(2)):
        @pl.when(is_older(b))
        def _():
            q = nn(mine.astype(BF16), ut[b])
            q = jnp.where(live[b], q, 0.0).astype(BF16)
            bmsg[b] = nn(q, vt[b])
            back_copy(b).start()

    def gather_copy(k):
        peer = peer_row(k)
        return remote(z_tile(row), z_tile(row), gsend.at[0], grecv.at[0], peer, col)

    def all_gathered():
        every = zfull.at[pl.ds(0, QB * (N_ROW - 1))]
        return remote(every, every, gsend.at[0], grecv.at[0], srow, scol)

    for k in range(1, N_ROW):
        gather_copy(k).start()

    wide = zfull[QB * row + div(col, 2)]
    root_out[...] = jnp.where(mod(col, 2) == 0, wide[:, :HALF], wide[:, HALF:])

    for b in range(2):
        @pl.when(is_older(b))
        def _():
            back_copy(b).wait_send()

    @pl.when(is_join)
    def _():
        remote(bjoin, bjoin, bjsend.at[0], brecv.at[0, 0], srow, scol).wait_send()

    @pl.when(is_s)
    def _():
        for da in range(1, NG):
            @pl.when(a + da < NG)
            def _():
                slots = brx.at[:, pl.ds(0, G)]
                remote(slots, slots, xsend.at[da - 1], xrecv.at[0], srow, scol).wait_send()
        for jj in range(G):
            def wait_z(count):
                slots = srx.at[jj, pl.ds(0, count)]
                remote(slots, slots, zsend.at[jj], zrecv.at[0], srow, scol).wait_send()

            pl.when(srel != jj)(lambda: wait_z(N_COL))
            pl.when(srel == jj)(lambda: wait_z(N_COL - 1))

    with jax.named_scope("gather_wait"):
        all_gathered().wait_recv()

    with jax.named_scope("final"):
        loads[8].wait()
        parts = [zfull[blocks_s[0, m]] for m in range(BB)]
        gathered = jnp.concatenate(parts, axis=1).astype(BF16)
        returned = nt(gathered, bt_v[...])
        child_out[0] = cx_v[...].astype(F32) - folded(nn(two_halves(returned), ci_v[...]))

    all_gathered().wait_send()


def per_device(
    root_rhs, diag_inv, tile_u, tile_v, tile_rank, child_x, border_t, child_inv, child_blocks
):
    vmem = pl.BlockSpec(memory_space=pltpu.VMEM)
    hbm = pl.BlockSpec(memory_space=pltpu.HBM)
    dma = pltpu.SemaphoreType.DMA
    pairs = G * (G - 1) // 2
    wide = (RHS, TILE)
    return pl.pallas_call(
        kernel,
        out_shape=(
            jax.ShapeDtypeStruct((RHS, HALF), F32),
            jax.ShapeDtypeStruct((1, RHS, TILE), F32),
        ),
        in_specs=[hbm] * 9,
        out_specs=(vmem, vmem),
        scratch_shapes=[
            pltpu.VMEM((RHS, G * TILE), BF16),
            pltpu.VMEM(wide, BF16),
            pltpu.SMEM((1, BB), jnp.int32),
            pltpu.SMEM((1, 2), jnp.int32),
            pltpu.VMEM((RMAX, TILE), F32),
            pltpu.VMEM((G, TILE, TILE), BF16),
            pltpu.VMEM((2, TILE, RMAX), BF16),
            pltpu.VMEM((2, RMAX, TILE), BF16),
            pltpu.VMEM((pairs, TILE, RMAX), BF16),
            pltpu.VMEM((G, TILE, RMAX), F32),
            pltpu.VMEM((G, RMAX, TILE), F32),
            pltpu.VMEM((G, TILE, RMAX), BF16),
            pltpu.VMEM((G, RMAX, TILE), BF16),
            pltpu.VMEM((G, RMAX, TILE), BF16),
            pltpu.VMEM((G, TILE, RMAX), BF16),
            pltpu.VMEM((G, *wide), F32),
            pltpu.VMEM((G, *wide), F32),
            pltpu.VMEM((TILE, BB * BLK), BF16),
            pltpu.VMEM((TILE, TILE), BF16),
            pltpu.VMEM((2, RMAX, TILE), BF16),
            pltpu.VMEM((2, TILE, RMAX), BF16),
            pltpu.VMEM((G, TILE, TILE), BF16),
            pltpu.VMEM((RMAX, TILE), F32),
            pltpu.VMEM((TILE, RMAX), F32),
            pltpu.VMEM((pairs, RMAX, TILE), F32),
            pltpu.VMEM((pairs, TILE, RMAX), F32),
            pltpu.VMEM((pairs, RMAX, TILE), BF16),
            pltpu.VMEM((pairs, RMAX, TILE), BF16),
            pltpu.VMEM((pairs, TILE, RMAX), BF16),
            pltpu.VMEM((NT, *wide), F32),
            pltpu.VMEM((N_ROW, *wide), F32),
            pltpu.VMEM((2, *wide), F32),
            pltpu.VMEM(wide, F32),
            pltpu.VMEM((G, N_COL, *wide), F32),
            pltpu.VMEM((G, *wide), F32),
            pltpu.VMEM((NT * QB, RHS, BLK), F32),
            pltpu.VMEM((G, QB, RHS, BLK), F32),
            pltpu.VMEM((2, *wide), F32),
            pltpu.VMEM((G, (NG - 1) * G, *wide), F32),
            pltpu.VMEM((G, *wide), F32),
            dma((9,)),
            dma((1,)),
            dma((1,)),
            dma((2,)),
            dma((2, pairs)),
            dma((1,)),
            dma((G,)),
            dma((NG - 1,)),
            dma((2,)),
            dma((G,)),
            dma((1,)),
            dma((2,)),
            dma((G, NG - 1)),
            dma((1,)),
            dma((1,)),
            dma((1,)),
            dma((1,)),
            dma((2, G)),
            dma((G,)),
            dma((1,)),
            dma((2,)),
        ],
        compiler_params=pltpu.CompilerParams(
            collective_id=0, has_side_effects=True, vmem_limit_bytes=48_000_000
        ),
    )(
        *(
            pltpu.with_memory_space_constraint(array, pltpu.HBM)
            for array in (
                root_rhs, child_x, child_blocks, tile_rank, diag_inv,
                tile_u, tile_v, border_t, child_inv,
            )
        )
    )


def solution(mesh):
    both = ("row", "col")
    tiles = P("row", "col", None, None, None, None)
    in_specs = (
        P(),
        P(),
        tiles,
        tiles,
        P("row", "col", None, None),
        P(both, None, None),
        P(both, None, None),
        P(both, None, None),
        P(both, None),
    )
    out_specs = (P(None, both), P(both, None, None))
    return jax.shard_map(
        per_device, mesh=mesh, in_specs=in_specs, out_specs=out_specs, check_vma=False
    )
```

```python
import jax
import jax.numpy as jnp
from jax import lax
from jax.experimental import pallas as pl
from jax.experimental.pallas import tpu as pltpu
from jax.sharding import PartitionSpec as P

MESH = pl.DeviceIdType.MESH
F32 = jnp.float32
BF16 = jnp.bfloat16
NT = 16
TILE = 512
RHS = 8
RMAX = 128
BLK = 128
BB = 8
N_ROW = 16
N_COL = 8
G = 4
NG = NT // G
SOLVER_ROW = (3, 3, 0, 1)
SOLVER_COL = (1, 3, 3, 3)
JOIN = 3
FAR_FIRST = (
    (2, 2), (3, 2), (0, 2), (2, 3), (3, 3), (0, 1), (2, 1), (3, 1), (0, 3),
    (1, 2), (3, 0), (1, 3), (1, 1), (2, 0), (1, 0),
)
NEAR_FIRST = (
    (1, 0), (3, 0), (0, 1), (2, 0), (1, 1), (3, 1), (0, 3), (2, 1), (1, 3), (3, 3),
    (0, 2), (2, 3), (1, 2), (3, 2), (2, 2),
)
SEND_ROWS = ((0, 2, 0), (1, 1, 2), (2, 0, 3), (3, 3, 1))
SEND_ORDER = (
    ((1, 0), (0, 0), (2, 0)),
    ((1, 1), (0, 1)),
    ((1, 2), (0, 2), (2, 1)),
    ((1, 3), (0, 3), (2, 2), (2, 3), (3, 0), (3, 1), (3, 2), (3, 3)),
)
SOURCE = (2, 0)
RELAY = (3, 3)
VIA = ((10, 8, (0, 1)), (14, 13, (5,)))
HALF = TILE // N_COL
QB = TILE // BLK


def div(x, n):
    return lax.div(x, jnp.int32(n))


def mod(x, n):
    return lax.rem(x, jnp.int32(n))


def pick(table, group):
    if isinstance(group, int):
        return jnp.int32(table[group])
    value = jnp.int32(table[-1])
    for g in range(len(table) - 1):
        value = jnp.where(group == g, jnp.int32(table[g]), value)
    return value


def solver_of(group):
    return G * group + pick(SOLVER_ROW, group), pick(SOLVER_COL, group)


def pair(i, j):
    return i * (i - 1) // 2 + j


def nn(a, b):
    return lax.dot_general(a, b, (((1,), (0,)), ((), ())), preferred_element_type=F32)


def nt(a, b):
    return lax.dot_general(a, b, (((1,), (1,)), ((), ())), preferred_element_type=F32)


def two_halves(t):
    hi = t.astype(BF16).astype(F32)
    return jnp.concatenate([hi, t - hi], axis=0).astype(BF16)


def folded(r):
    return r[:RHS] + r[RHS:]


def kernel(
    rhs_hbm, cx_hbm, blocks_hbm, rank_hbm, diag_hbm, u_hbm, v_hbm, bt_hbm, ci_hbm,
    root_out, child_out,
    rhs_v, cx_v, blocks_s, rank_s, urelay, dt, ut, vt, utin,
    vjoin, ujoin, vj, uj, vjt, ujt, xjoin, bjoin,
    bt_v, ci_v, u_v, v_v, d_v, us, vs, urx, vrx, wf, wb, vbf,
    childp, childrx, xrx, rowmsg, srx, xs, zfull, zs, bmsg, brx, tacc,
    lsem, csend, crecv, tsend, trecv, msend, srecv, xsend, xrecv,
    zsend, zrecv, bsend, brecv, gsend, grecv, rsend, rrecv, jtile, xjrecv, bjsend, viarecv,
):
    row = lax.axis_index("row")
    col = lax.axis_index("col")
    a = div(row, G)
    ii = mod(row, G)
    half = div(col, G)
    jcol = mod(col, G)
    srow, scol = solver_of(a)
    srel = srow - G * a
    is_s = (row == srow) & (col == scol)
    ours = G * mod(a, 2)
    near = mod(a + 1, 2)
    is_join = (col == JOIN) & (a > 0)
    lends = (half == near) & (a > 0)
    via_source = row < 0
    is_via = row < 0
    via_row = jnp.int32(VIA[-1][1])
    for start, stop, columns in VIA:
        for c in columns:
            via_source = via_source | ((row == start) & (col == c))
            is_via = is_via | ((row == stop) & (col == c))
        via_row = jnp.where(row == start, jnp.int32(stop), via_row)
    is_source = (row == SOURCE[0]) & (col == SOURCE[1])
    is_relay = (row == RELAY[0]) & (col == RELAY[1])

    width = G * TILE
    loads = [
        pltpu.make_async_copy(bt_hbm.at[0], bt_v, lsem.at[0]),
        pltpu.make_async_copy(cx_hbm.at[0], cx_v, lsem.at[1]),
        pltpu.make_async_copy(blocks_hbm, blocks_s, lsem.at[2]),
        pltpu.make_async_copy(rank_hbm.at[0, 0], rank_s, lsem.at[3]),
        pltpu.make_async_copy(u_hbm.at[0, 0, 0], u_v, lsem.at[4]),
        pltpu.make_async_copy(v_hbm.at[0, 0, 0], v_v, lsem.at[5]),
        pltpu.make_async_copy(
            rhs_hbm.at[:, pl.ds(pl.multiple_of(width * a, width), width)], rhs_v, lsem.at[6]
        ),
        pltpu.make_async_copy(diag_hbm.at[pl.ds(G * a, G)], d_v, lsem.at[7]),
        pltpu.make_async_copy(ci_hbm.at[0], ci_v, lsem.at[8]),
    ]
    for load in loads:
        load.start()

    def remote(src, dst, send, recv, r, c):
        return pltpu.make_async_remote_copy(
            src_ref=src, dst_ref=dst, send_sem=send, recv_sem=recv,
            device_id=(r, c), device_id_type=MESH,
        )

    bar = pltpu.get_barrier_semaphore()

    def signal(r, c):
        pl.semaphore_signal(bar, inc=1, device_id=(r, c), device_id_type=MESH)

    for k in range(1, N_ROW):
        signal(mod(row + k, N_ROW), col)

    @pl.when(jnp.logical_not(is_s))
    def _():
        signal(srow, scol)

    for b in range(2):
        @pl.when(half + 2 * b < a)
        def _():
            signal(*solver_of(half + 2 * b))

    @pl.when(is_s)
    def _():
        me = ii * N_COL + col
        for k in range(1, G * N_COL):
            other = mod(me + k, G * N_COL)
            signal(G * a + div(other, N_COL), mod(other, N_COL))
        for da in range(1, NG):
            @pl.when(a + da < NG)
            def _():
                for n in range(G * G):
                    signal(G * (a + da) + n // G, ours + n % G)

    @pl.when(lends & (col != JOIN))
    def _():
        signal(row, jnp.int32(JOIN))

    @pl.when(is_join)
    def _():
        for jj in range(G):
            c = G * near + jj
            pl.when(c != JOIN)(lambda: signal(row, c))
        signal(*solver_of(a - 1))

    @pl.when(is_s & (a + 1 < NG))
    def _():
        for i2 in range(G):
            signal(G * (a + 1) + i2, jnp.int32(JOIN))

    @pl.when(is_source)
    def _():
        signal(jnp.int32(RELAY[0]), jnp.int32(RELAY[1]))

    @pl.when(is_relay)
    def _():
        signal(jnp.int32(SOURCE[0]), jnp.int32(SOURCE[1]))

    greeted = (
        N_ROW - 1
        + jnp.where(is_source | is_relay, 1, 0)
        + jnp.where(lends & (col != JOIN), 1, 0)
        + jnp.where(is_join, G + 1 - jnp.where(lends, 1, 0), 0)
        + jnp.where(is_s & (a + 1 < NG), G, 0)
        + jnp.where(is_s, G * N_COL - 1 + G * G * (NG - 1 - a), 1)
        + jnp.where(half < a, 1, 0)
        + jnp.where(half + 2 < a, 1, 0)
    )

    lane = lax.broadcasted_iota(jnp.int32, (RHS, RMAX), 1)
    loads[3].wait()
    live = [lane < rank_s[0, b] for b in range(2)]

    with jax.named_scope("up"):
        loads[1].wait()
        loads[2].wait()
        loads[0].wait()
        up = nn(cx_v[...], bt_v[...])
        pieces = [up[:, m * BLK:(m + 1) * BLK] for m in range(BB)]
        ids = [jnp.full((RHS, BLK), blocks_s[0, m], jnp.int32) for m in range(BB)]

        @pl.loop(0, NT)
        def _(r):
            for q in range(QB):
                block = jnp.zeros((RHS, BLK), F32)
                for m in range(BB):
                    block = block + jnp.where(ids[m] == r * (QB) + q, pieces[m], 0.0)
                childp[r, :, q * BLK:(q + 1) * BLK] = block

    loads[4].wait()
    loads[5].wait()
    slot = div(a, 2)
    owner = (half == mod(a, 2)) & (jcol < ii)
    t_idx = div(ii * (ii - 1), 2) + jcol
    own_tile = jnp.where(owner & is_s, t_idx, -1)
    own_lent = lends & is_join
    from_slot = jnp.where(lends, div(a + 1, 2) - 1, slot)

    @pl.when(owner | lends)
    def _():
        us[...] = u_v[from_slot].astype(F32)
        wide = lax.broadcasted_iota(jnp.int32, (TILE, RMAX), 1)
        vs[...] = jnp.where(wide < rank_s[0, from_slot], v_v[from_slot].astype(F32), 0.0)

    @pl.when(owner & is_s)
    def _():
        urx[t_idx] = us[...]
        vrx[t_idx] = vs[...]

    @pl.when(own_lent)
    def _():
        ujoin[jcol] = us[...]
        vjoin[jcol] = vs[...]

    with jax.named_scope("bar"):
        pl.semaphore_wait(bar, greeted)

    def peer_row(order, k):
        dy, dz = order[k - 1]
        return G * mod(a + dy, NG) + mod(ii + dz, G)

    def child_copy(k):
        peer = peer_row(FAR_FIRST, k)
        return remote(childp.at[peer], childrx.at[k - 1], csend.at[0], crecv.at[0], peer, col)

    def all_children():
        every = pl.ds(0, N_ROW - 1)
        return remote(
            childp.at[every], childrx.at[every], csend.at[0], crecv.at[0], srow, scol
        )

    def v_copy():
        return remote(vs, vrx.at[t_idx], tsend.at[0], trecv.at[0, t_idx], srow, scol)

    def u_copy():
        return remote(us, urx.at[t_idx], tsend.at[1], trecv.at[1, t_idx], srow, scol)

    def relay_in():
        return remote(
            us, urelay, tsend.at[1], rrecv.at[0], jnp.int32(RELAY[0]), jnp.int32(RELAY[1])
        )

    def relay_out():
        t = pair(*SOURCE)
        return remote(urelay, urx.at[t], rsend.at[0], trecv.at[1, t], srow, scol)

    def lend_copy(n, src, dst):
        return remote(
            src, dst.at[jcol], tsend.at[n], jtile.at[n, jcol], row, jnp.int32(JOIN)
        )

    lends_out = lends & (col != JOIN)
    def via_in(n, ref):
        return remote(
            ref, ref, tsend.at[n], viarecv.at[n], via_row, col
        )

    def via_out(n, ref, dst):
        t = pair(2, 0) + jcol
        return remote(ref, dst.at[t], tsend.at[n], trecv.at[n, t], srow, scol)

    sends_tile = owner & jnp.logical_not(is_s | via_source)
    sends_u = sends_tile & jnp.logical_not(is_source)
    pl.when(is_source)(lambda: relay_in().start())
    for k in range(1, N_ROW):
        child_copy(k).start()
    pl.when(sends_tile)(lambda: v_copy().start())
    pl.when(sends_u)(lambda: u_copy().start())

    @pl.when(via_source)
    def _():
        via_in(0, vs).start()
        via_in(1, us).start()

    @pl.when(lends_out)
    def _():
        lend_copy(0, vs, vjoin).start()
        lend_copy(1, us, ujoin).start()

    with jax.named_scope("child_wait"):
        all_children().wait_recv()
        total = childp[row]
        for k in range(N_ROW - 1):
            total = total + childrx[k]
        rowmsg[...] = total

    @pl.when(is_via)
    def _():
        via_in(0, vs).wait_recv()
        via_out(0, vs, vrx).start()
        via_in(1, us).wait_recv()
        via_out(1, us, urx).start()

    tiles = [(i, j) for i in range(G) for j in range(i)]

    def turn():
        with jax.named_scope("turn"):
            for jj in range(G):
                dt[jj] = d_v[jj].T
            for i, j in tiles:
                t = pair(i, j)
                utin[t] = urx[t].T.astype(BF16)
                wb[t] = nn(vrx[t].T.astype(BF16), dt[j]).astype(BF16)

    loads[7].wait()

    @pl.when(is_s)
    def _():
        with jax.named_scope("tiles_wait"):
            for i, j in ((3, 1), (3, 0), (3, 2), (1, 0), (2, 0), (2, 1)):
                t = pair(i, j)

                @pl.when(own_tile != t)
                def _():
                    with jax.named_scope(f"tv{i}{j}"):
                        remote(vs, vrx.at[t], tsend.at[0], trecv.at[0, t], srow, scol).wait_recv()
                    with jax.named_scope(f"tu{i}{j}"):
                        remote(us, urx.at[t], tsend.at[1], trecv.at[1, t], srow, scol).wait_recv()

                vbf[t] = vrx[t].astype(BF16)
                wf[t] = nn(urx[t].astype(BF16), d_v[i]).astype(BF16)
        pl.when(a == NG - 1)(turn)

    def is_older(b):
        return half + 2 * b + 1 < a

    with jax.named_scope("turn2"):
        for b in range(2):
            @pl.when(is_older(b))
            def _():
                ut[b] = u_v[b].T
                vt[b] = v_v[b].T

        @pl.when(is_join)
        def _():
            for jj in range(G):
                @pl.when(G * near + jj != JOIN)
                def _():
                    remote(
                        vs, vjoin.at[jj], tsend.at[0], jtile.at[0, jj], row, jnp.int32(0)
                    ).wait_recv()
                    remote(
                        us, ujoin.at[jj], tsend.at[1], jtile.at[1, jj], row, jnp.int32(0)
                    ).wait_recv()

                vj[jj] = vjoin[jj].astype(BF16)
                uj[jj] = ujoin[jj].astype(BF16)
                vjt[jj] = vjoin[jj].T.astype(BF16)
                ujt[jj] = ujoin[jj].T.astype(BF16)

    with jax.named_scope("fwd_row"):
        for b in range(2):
            @pl.when(is_older(b))
            def _():
                remote(xs.at[0], xrx.at[b], xsend.at[0], xrecv.at[b], srow, scol).wait_recv()
                p = nn(xrx[b].astype(BF16), v_v[b])
                p = jnp.where(live[b], p, 0.0).astype(BF16)
                rowmsg[...] += nn(p, u_v[b])

        @pl.when(is_join)
        def _():
            for jj in range(G):
                remote(
                    xs.at[0], xjoin.at[jj], xsend.at[0], xjrecv.at[jj], srow, scol
                ).wait_recv()
                p = nn(xjoin[jj].astype(BF16), vj[jj]).astype(BF16)
                rowmsg[...] += nn(p, uj[jj])

    def row_copy():
        return remote(
            rowmsg, srx.at[ii, col], msend.at[0], srecv.at[ii], srow, scol
        )

    @pl.when(is_s)
    def _():
        srx[ii, col] = rowmsg[...]

    @pl.when(jnp.logical_not(is_s))
    def _():
        row_copy().start()

    @pl.when(is_relay)
    def _():
        relay_in().wait_recv()
        relay_out().start()

    loads[6].wait()

    def x_copy(jj, da, i2):
        if da == 1:
            return remote(
                xs.at[jj], xjoin.at[jj], xsend.at[0], xjrecv.at[jj],
                G * (a + 1) + i2, jnp.int32(JOIN),
            )
        return remote(
            xs.at[jj], xrx.at[slot], xsend.at[da - 1], xrecv.at[slot],
            G * (a + da) + i2, ours + jj,
        )

    @pl.when(is_s)
    def _():
        def wait_row(jj, count):
            slots = srx.at[jj, pl.ds(0, count)]
            remote(slots, slots, msend.at[0], srecv.at[jj], srow, scol).wait_recv()

        def wait_all(jj):
            with jax.named_scope(f"s_fwd_wait{jj}"):
                pl.when(srel != jj)(lambda: wait_row(jj, N_COL))
                pl.when(srel == jj)(lambda: wait_row(jj, N_COL - 1))

        def base(jj):
            parts = [srx[jj, c] for c in range(N_COL)]
            while len(parts) > 1:
                parts = [parts[n] + parts[n + 1] for n in range(0, len(parts), 2)]
            right = rhs_v[:, jj * TILE:(jj + 1) * TILE].astype(F32) - parts[0]
            return folded(nn(two_halves(right), d_v[jj]))

        x = [None] * G

        send_rows = [pick(rows, a) for rows in SEND_ROWS]

        def publish(jj):
            xs[jj] = x[jj]

            @pl.when(a + 1 < NG)
            def _():
                for rank, j2 in SEND_ORDER[jj]:
                    x_copy(j2, 1, send_rows[rank]).start()

        wait_all(0)
        x[0] = base(0)
        publish(0)
        for jj in range(1, G):
            wait_all(jj)
            done = x[jj - 1].astype(BF16)
            for mm in range(jj, G):
                t = pair(mm, jj - 1)
                part = nn(nn(done, vbf[t]).astype(BF16), wf[t])
                x[mm] = part if x[mm] is None else x[mm] + part
            x[jj] = base(jj) - x[jj]
            publish(jj)
        for da in range(2, NG):
            @pl.when(a + da < NG)
            def _():
                for i2 in range(G):
                    for jj in range(G):
                        x_copy(jj, da, i2).start()
        pl.when(a < NG - 1)(turn)

    all_children().wait_send()
    @pl.when(via_source)
    def _():
        via_in(0, vs).wait_send()
        via_in(1, us).wait_send()

    @pl.when(is_via)
    def _():
        via_out(0, vs, vrx).wait_send()
        via_out(1, us, urx).wait_send()

    @pl.when(lends_out)
    def _():
        lend_copy(0, vs, vjoin).wait_send()
        lend_copy(1, us, ujoin).wait_send()

    pl.when(sends_tile)(lambda: v_copy().wait_send())
    pl.when(sends_u)(lambda: u_copy().wait_send())
    pl.when(is_source)(lambda: relay_in().wait_send())
    pl.when(is_relay)(lambda: relay_out().wait_send())
    pl.when(jnp.logical_not(is_s))(lambda: row_copy().wait_send())

    def z_tile(i):
        return zfull.at[pl.ds(QB * i, QB)]

    def z_copy(jj, k):
        c = mod(JOIN + k, N_COL)
        return c, remote(
            zs.at[jj], z_tile(G * a + jj), zsend.at[jj], zrecv.at[0], G * a + jj, c
        )

    may_be_own = {(SOLVER_COL[g] - JOIN) % N_COL for g in range(NG)}

    @pl.when(is_s)
    def _():
        def wait_da(jj, da):
            slots = brx.at[jj, pl.ds((da - 1) * G, G)]
            remote(slots, slots, bsend.at[0], brecv.at[jj, da - 1], srow, scol).wait_recv()

        def take(jj, da):
            n = (da - 1) * G
            tacc[jj] -= (brx[jj, n] + brx[jj, n + 1]) + (brx[jj, n + 2] + brx[jj, n + 3])

        def collect(rows, das):
            for da in das:
                @pl.when(a + da < NG)
                def _():
                    for jj in rows:
                        wait_da(jj, da)
                    for jj in rows:
                        take(jj, da)

        def base(jj):
            return folded(nn(two_halves(tacc[jj]), dt[jj]))

        z = [None] * G

        def publish(jj):
            for q in range(QB):
                part = z[jj][:, q * BLK:(q + 1) * BLK]
                zs[jj, q] = part
                zfull[QB * (G * a + jj) + q] = part
            for k in range(N_COL):
                c, copy = z_copy(jj, k)
                if k in may_be_own:
                    pl.when((srel != jj) | (c != col))(copy.start)
                else:
                    copy.start()

        tacc[...] = xs[...]
        with jax.named_scope("s_bwd_old"):
            collect(range(G), range(NG - 1, 1, -1))
        last = G - 1
        with jax.named_scope("s_bwd_wait3"):
            collect((last,), (1,))
        z[last] = base(last)
        publish(last)
        for jj in range(last - 1, -1, -1):
            with jax.named_scope(f"s_bwd_wait{jj}"):
                collect((jj,), (1,))
            done = z[jj + 1].astype(BF16)
            for mm in range(jj, -1, -1):
                t = pair(jj + 1, mm)
                part = nn(nn(done, utin[t]).astype(BF16), wb[t])
                z[mm] = part if z[mm] is None else z[mm] + part
            z[jj] = base(jj) - z[jj]
            publish(jj)

    @pl.when(jnp.logical_not(is_s))
    def _():
        with jax.named_scope("z_wait"):
            remote(zs.at[0], z_tile(row), zsend.at[0], zrecv.at[0], srow, scol).wait_recv()

    def back_copy(b):
        g = half + 2 * b
        n = (a - g - 1) * G + ii
        return remote(
            bmsg.at[b], brx.at[jcol, n], bsend.at[b], brecv.at[jcol, a - g - 1], *solver_of(g)
        )

    def join_copy(jj):
        return remote(
            bjoin.at[jj], brx.at[jj, ii], bjsend.at[0], brecv.at[jj, 0], *solver_of(a - 1)
        )

    @pl.when(is_join)
    def _():
        zb = jnp.concatenate([zfull[QB * row + q] for q in range(QB)], axis=1).astype(BF16)
        for jj in reversed(range(G)):
            bjoin[jj] = nn(nn(zb, ujt[jj]).astype(BF16), vjt[jj])
            join_copy(jj).start()

    mine = jnp.concatenate([zfull[QB * row + q] for q in range(QB)], axis=1)
    for b in reversed(range(2)):
        @pl.when(is_older(b))
        def _():
            q = nn(mine.astype(BF16), ut[b])
            q = jnp.where(live[b], q, 0.0).astype(BF16)
            bmsg[b] = nn(q, vt[b])
            back_copy(b).start()

    def gather_copy(k):
        peer = peer_row(NEAR_FIRST, k)
        return remote(z_tile(row), z_tile(row), gsend.at[0], grecv.at[0], peer, col)

    def all_gathered():
        every = zfull.at[pl.ds(0, QB * (N_ROW - 1))]
        return remote(every, every, gsend.at[0], grecv.at[0], srow, scol)

    for k in range(1, N_ROW):
        gather_copy(k).start()

    wide = zfull[QB * row + div(col, 2)]
    root_out[...] = jnp.where(mod(col, 2) == 0, wide[:, :HALF], wide[:, HALF:])

    for b in range(2):
        @pl.when(is_older(b))
        def _():
            back_copy(b).wait_send()

    @pl.when(is_join)
    def _():
        remote(bjoin, bjoin, bjsend.at[0], brecv.at[0, 0], srow, scol).wait_send()

    @pl.when(is_s)
    def _():
        for da in range(1, NG):
            @pl.when(a + da < NG)
            def _():
                slots = brx.at[:, pl.ds(0, G)]
                remote(slots, slots, xsend.at[da - 1], xrecv.at[0], srow, scol).wait_send()
        for jj in range(G):
            def wait_z(count):
                slots = srx.at[jj, pl.ds(0, count)]
                remote(slots, slots, zsend.at[jj], zrecv.at[0], srow, scol).wait_send()

            pl.when(srel != jj)(lambda: wait_z(N_COL))
            pl.when(srel == jj)(lambda: wait_z(N_COL - 1))

    with jax.named_scope("gather_wait"):
        all_gathered().wait_recv()

    with jax.named_scope("final"):
        loads[8].wait()
        parts = [zfull[blocks_s[0, m]] for m in range(BB)]
        gathered = jnp.concatenate(parts, axis=1).astype(BF16)
        returned = nt(gathered, bt_v[...])
        child_out[0] = cx_v[...].astype(F32) - folded(nn(two_halves(returned), ci_v[...]))

    all_gathered().wait_send()


def per_device(
    root_rhs, diag_inv, tile_u, tile_v, tile_rank, child_x, border_t, child_inv, child_blocks
):
    vmem = pl.BlockSpec(memory_space=pltpu.VMEM)
    hbm = pl.BlockSpec(memory_space=pltpu.HBM)
    dma = pltpu.SemaphoreType.DMA
    pairs = G * (G - 1) // 2
    wide = (RHS, TILE)
    return pl.pallas_call(
        kernel,
        out_shape=(
            jax.ShapeDtypeStruct((RHS, HALF), F32),
            jax.ShapeDtypeStruct((1, RHS, TILE), F32),
        ),
        in_specs=[hbm] * 9,
        out_specs=(vmem, vmem),
        scratch_shapes=[
            pltpu.VMEM((RHS, G * TILE), BF16),
            pltpu.VMEM(wide, BF16),
            pltpu.SMEM((1, BB), jnp.int32),
            pltpu.SMEM((1, 2), jnp.int32),
            pltpu.VMEM((RMAX, TILE), F32),
            pltpu.VMEM((G, TILE, TILE), BF16),
            pltpu.VMEM((2, TILE, RMAX), BF16),
            pltpu.VMEM((2, RMAX, TILE), BF16),
            pltpu.VMEM((pairs, TILE, RMAX), BF16),
            pltpu.VMEM((G, TILE, RMAX), F32),
            pltpu.VMEM((G, RMAX, TILE), F32),
            pltpu.VMEM((G, TILE, RMAX), BF16),
            pltpu.VMEM((G, RMAX, TILE), BF16),
            pltpu.VMEM((G, RMAX, TILE), BF16),
            pltpu.VMEM((G, TILE, RMAX), BF16),
            pltpu.VMEM((G, *wide), F32),
            pltpu.VMEM((G, *wide), F32),
            pltpu.VMEM((TILE, BB * BLK), BF16),
            pltpu.VMEM((TILE, TILE), BF16),
            pltpu.VMEM((2, RMAX, TILE), BF16),
            pltpu.VMEM((2, TILE, RMAX), BF16),
            pltpu.VMEM((G, TILE, TILE), BF16),
            pltpu.VMEM((RMAX, TILE), F32),
            pltpu.VMEM((TILE, RMAX), F32),
            pltpu.VMEM((pairs, RMAX, TILE), F32),
            pltpu.VMEM((pairs, TILE, RMAX), F32),
            pltpu.VMEM((pairs, RMAX, TILE), BF16),
            pltpu.VMEM((pairs, RMAX, TILE), BF16),
            pltpu.VMEM((pairs, TILE, RMAX), BF16),
            pltpu.VMEM((NT, *wide), F32),
            pltpu.VMEM((N_ROW, *wide), F32),
            pltpu.VMEM((2, *wide), F32),
            pltpu.VMEM(wide, F32),
            pltpu.VMEM((G, N_COL, *wide), F32),
            pltpu.VMEM((G, *wide), F32),
            pltpu.VMEM((NT * QB, RHS, BLK), F32),
            pltpu.VMEM((G, QB, RHS, BLK), F32),
            pltpu.VMEM((2, *wide), F32),
            pltpu.VMEM((G, (NG - 1) * G, *wide), F32),
            pltpu.VMEM((G, *wide), F32),
            dma((9,)),
            dma((1,)),
            dma((1,)),
            dma((2,)),
            dma((2, pairs)),
            dma((1,)),
            dma((G,)),
            dma((NG - 1,)),
            dma((2,)),
            dma((G,)),
            dma((1,)),
            dma((2,)),
            dma((G, NG - 1)),
            dma((1,)),
            dma((1,)),
            dma((1,)),
            dma((1,)),
            dma((2, G)),
            dma((G,)),
            dma((1,)),
            dma((2,)),
        ],
        compiler_params=pltpu.CompilerParams(
            collective_id=0, has_side_effects=True, vmem_limit_bytes=48_000_000
        ),
    )(
        *(
            pltpu.with_memory_space_constraint(array, pltpu.HBM)
            for array in (
                root_rhs, child_x, child_blocks, tile_rank, diag_inv,
                tile_u, tile_v, border_t, child_inv,
            )
        )
    )


def solution(mesh):
    both = ("row", "col")
    tiles = P("row", "col", None, None, None, None)
    in_specs = (
        P(),
        P(),
        tiles,
        tiles,
        P("row", "col", None, None),
        P(both, None, None),
        P(both, None, None),
        P(both, None, None),
        P(both, None),
    )
    out_specs = (P(None, both), P(both, None, None))
    return jax.shard_map(
        per_device, mesh=mesh, in_specs=in_specs, out_specs=out_specs, check_vma=False
    )
```

```python
import jax
import jax.numpy as jnp
from jax import lax
from jax.experimental import pallas as pl
from jax.experimental.pallas import tpu as pltpu
from jax.sharding import PartitionSpec as P

MESH = pl.DeviceIdType.MESH
F32 = jnp.float32
BF16 = jnp.bfloat16
NT = 16
TILE = 512
RHS = 8
RMAX = 128
BLK = 128
BB = 8
N_ROW = 16
N_COL = 8
G = 4
NG = NT // G
SOLVER_ROW = (3, 3, 0, 1)
SOLVER_COL = (1, 3, 3, 3)
JOIN = 3
FAR_FIRST = (
    (2, 2), (3, 2), (0, 2), (2, 3), (3, 3), (0, 1), (2, 1), (3, 1), (0, 3),
    (1, 2), (3, 0), (1, 3), (1, 1), (2, 0), (1, 0),
)
NEAR_FIRST = (
    (1, 0), (3, 0), (0, 1), (2, 0), (1, 1), (3, 1), (0, 3), (2, 1), (1, 3), (3, 3),
    (0, 2), (2, 3), (1, 2), (3, 2), (2, 2),
)
SEND_ROWS = ((0, 2, 0), (1, 1, 2), (2, 0, 3), (3, 3, 1))
SEND_ORDER = (
    ((1, 0), (0, 0), (2, 0)),
    ((1, 1), (0, 1)),
    ((1, 2), (0, 2), (2, 1)),
    ((1, 3), (0, 3), (2, 2), (2, 3), (3, 0), (3, 1), (3, 2), (3, 3)),
)
SOURCE = (2, 0)
RELAY = (3, 3)
VIA = ((10, 8, (0, 1)), (14, 13, (5,)))
HALF = TILE // N_COL
QB = TILE // BLK


def div(x, n):
    return lax.div(x, jnp.int32(n))


def mod(x, n):
    return lax.rem(x, jnp.int32(n))


def pick(table, group):
    if isinstance(group, int):
        return jnp.int32(table[group])
    value = jnp.int32(table[-1])
    for g in range(len(table) - 1):
        value = jnp.where(group == g, jnp.int32(table[g]), value)
    return value


def solver_of(group):
    return G * group + pick(SOLVER_ROW, group), pick(SOLVER_COL, group)


def pair(i, j):
    return i * (i - 1) // 2 + j


def nn(a, b):
    return lax.dot_general(a, b, (((1,), (0,)), ((), ())), preferred_element_type=F32)


def nt(a, b):
    return lax.dot_general(a, b, (((1,), (1,)), ((), ())), preferred_element_type=F32)


def two_halves(t):
    hi = t.astype(BF16).astype(F32)
    return jnp.concatenate([hi, t - hi], axis=0).astype(BF16)


def folded(r):
    return r[:RHS] + r[RHS:]


def kernel(
    rhs_hbm, cx_hbm, blocks_hbm, rank_hbm, diag_hbm, u_hbm, v_hbm, bt_hbm, ci_hbm,
    root_out, child_out,
    rhs_v, cx_v, blocks_s, rank_s, urelay, dt, ut, vt, utin,
    vjoin, ujoin, vj, uj, vjt, ujt, xjoin, bjoin,
    bt_v, ci_v, u_v, v_v, d_v, us, vs, urx, vrx, wf, wb, vbf,
    childp, childrx, xrx, rowmsg, srx, xs, zfull, zs, bmsg, brx, tacc,
    lsem, csend, crecv, tsend, trecv, msend, srecv, xsend, xrecv,
    zsend, zrecv, bsend, brecv, gsend, grecv, rsend, rrecv, jtile, xjrecv, bjsend, viarecv, back,
):
    row = lax.axis_index("row")
    col = lax.axis_index("col")
    a = div(row, G)
    ii = mod(row, G)
    half = div(col, G)
    jcol = mod(col, G)
    srow, scol = solver_of(a)
    srel = srow - G * a
    is_s = (row == srow) & (col == scol)
    ours = G * mod(a, 2)
    near = mod(a + 1, 2)
    is_join = (col == JOIN) & (a > 0)
    lends = (half == near) & (a > 0)
    via_source = row < 0
    is_via = row < 0
    via_row = jnp.int32(VIA[-1][1])
    for start, stop, columns in VIA:
        for c in columns:
            via_source = via_source | ((row == start) & (col == c))
            is_via = is_via | ((row == stop) & (col == c))
        via_row = jnp.where(row == start, jnp.int32(stop), via_row)
    is_source = (row == SOURCE[0]) & (col == SOURCE[1])
    is_relay = (row == RELAY[0]) & (col == RELAY[1])

    width = G * TILE
    loads = [
        pltpu.make_async_copy(bt_hbm.at[0], bt_v, lsem.at[0]),
        pltpu.make_async_copy(cx_hbm.at[0], cx_v, lsem.at[1]),
        pltpu.make_async_copy(blocks_hbm, blocks_s, lsem.at[2]),
        pltpu.make_async_copy(rank_hbm.at[0, 0], rank_s, lsem.at[3]),
        pltpu.make_async_copy(u_hbm.at[0, 0, 0], u_v, lsem.at[4]),
        pltpu.make_async_copy(v_hbm.at[0, 0, 0], v_v, lsem.at[5]),
        pltpu.make_async_copy(
            rhs_hbm.at[:, pl.ds(pl.multiple_of(width * a, width), width)], rhs_v, lsem.at[6]
        ),
        pltpu.make_async_copy(diag_hbm.at[pl.ds(G * a, G)], d_v, lsem.at[7]),
        pltpu.make_async_copy(ci_hbm.at[0], ci_v, lsem.at[8]),
    ]
    for load in loads:
        load.start()

    def remote(src, dst, send, recv, r, c):
        return pltpu.make_async_remote_copy(
            src_ref=src, dst_ref=dst, send_sem=send, recv_sem=recv,
            device_id=(r, c), device_id_type=MESH,
        )

    bar = pltpu.get_barrier_semaphore()

    def signal(r, c):
        pl.semaphore_signal(bar, inc=1, device_id=(r, c), device_id_type=MESH)

    for k in range(1, N_ROW):
        signal(mod(row + k, N_ROW), col)

    @pl.when(jnp.logical_not(is_s))
    def _():
        signal(srow, scol)

    for b in range(2):
        @pl.when(half + 2 * b < a)
        def _():
            signal(*solver_of(half + 2 * b))

    @pl.when(is_s)
    def _():
        me = ii * N_COL + col
        for k in range(1, G * N_COL):
            other = mod(me + k, G * N_COL)
            signal(G * a + div(other, N_COL), mod(other, N_COL))
        for da in range(1, NG):
            @pl.when(a + da < NG)
            def _():
                for n in range(G * G):
                    signal(G * (a + da) + n // G, ours + n % G)

    @pl.when(lends & (col != JOIN))
    def _():
        signal(row, jnp.int32(JOIN))

    @pl.when(is_join)
    def _():
        for jj in range(G):
            c = G * near + jj
            pl.when(c != JOIN)(lambda: signal(row, c))
        signal(*solver_of(a - 1))

    @pl.when(is_s & (a + 1 < NG))
    def _():
        for i2 in range(G):
            signal(G * (a + 1) + i2, jnp.int32(JOIN))

    @pl.when(is_source)
    def _():
        signal(jnp.int32(RELAY[0]), jnp.int32(RELAY[1]))

    @pl.when(is_relay)
    def _():
        signal(jnp.int32(SOURCE[0]), jnp.int32(SOURCE[1]))

    greeted = (
        N_ROW - 1
        + jnp.where(is_source | is_relay, 1, 0)
        + jnp.where(lends & (col != JOIN), 1, 0)
        + jnp.where(is_join, G + 1 - jnp.where(lends, 1, 0), 0)
        + jnp.where(is_s & (a + 1 < NG), G, 0)
        + jnp.where(is_s, G * N_COL - 1 + G * G * (NG - 1 - a), 1)
        + jnp.where(half < a, 1, 0)
        + jnp.where(half + 2 < a, 1, 0)
    )

    lane = lax.broadcasted_iota(jnp.int32, (RHS, RMAX), 1)
    loads[3].wait()
    live = [lane < rank_s[0, b] for b in range(2)]

    with jax.named_scope("up"):
        loads[1].wait()
        loads[2].wait()
        loads[0].wait()
        up = nn(cx_v[...], bt_v[...])
        pieces = [up[:, m * BLK:(m + 1) * BLK] for m in range(BB)]
        ids = [jnp.full((RHS, BLK), blocks_s[0, m], jnp.int32) for m in range(BB)]

        @pl.loop(0, NT)
        def _(r):
            for q in range(QB):
                block = jnp.zeros((RHS, BLK), F32)
                for m in range(BB):
                    block = block + jnp.where(ids[m] == r * (QB) + q, pieces[m], 0.0)
                childp[r, :, q * BLK:(q + 1) * BLK] = block

    loads[4].wait()
    loads[5].wait()
    slot = div(a, 2)
    owner = (half == mod(a, 2)) & (jcol < ii)
    t_idx = div(ii * (ii - 1), 2) + jcol
    own_tile = jnp.where(owner & is_s, t_idx, -1)
    own_lent = lends & is_join
    from_slot = jnp.where(lends, div(a + 1, 2) - 1, slot)

    @pl.when(owner | lends)
    def _():
        us[...] = u_v[from_slot].astype(F32)
        wide = lax.broadcasted_iota(jnp.int32, (TILE, RMAX), 1)
        vs[...] = jnp.where(wide < rank_s[0, from_slot], v_v[from_slot].astype(F32), 0.0)

    @pl.when(owner & is_s)
    def _():
        urx[t_idx] = us[...]
        vrx[t_idx] = vs[...]

    @pl.when(own_lent)
    def _():
        ujoin[jcol] = us[...]
        vjoin[jcol] = vs[...]

    with jax.named_scope("bar"):
        pl.semaphore_wait(bar, greeted)

    def peer_row(order, k):
        dy, dz = order[k - 1]
        return G * mod(a + dy, NG) + mod(ii + dz, G)

    def child_copy(k):
        peer = peer_row(FAR_FIRST, k)
        return remote(childp.at[peer], childrx.at[k - 1], csend.at[0], crecv.at[0], peer, col)

    def all_children():
        every = pl.ds(0, N_ROW - 1)
        return remote(
            childp.at[every], childrx.at[every], csend.at[0], crecv.at[0], srow, scol
        )

    def v_copy():
        return remote(vs, vrx.at[t_idx], tsend.at[0], trecv.at[0, t_idx], srow, scol)

    def u_copy():
        return remote(us, urx.at[t_idx], tsend.at[1], trecv.at[1, t_idx], srow, scol)

    def relay_in():
        return remote(
            us, urelay, tsend.at[1], rrecv.at[0], jnp.int32(RELAY[0]), jnp.int32(RELAY[1])
        )

    def relay_out():
        t = pair(*SOURCE)
        return remote(urelay, urx.at[t], rsend.at[0], trecv.at[1, t], srow, scol)

    def lend_copy(n, src, dst):
        return remote(
            src, dst.at[jcol], tsend.at[n], jtile.at[n, jcol], row, jnp.int32(JOIN)
        )

    lends_out = lends & (col != JOIN)
    def via_in(n, ref):
        return remote(
            ref, ref, tsend.at[n], viarecv.at[n], via_row, col
        )

    def via_out(n, ref, dst):
        t = pair(2, 0) + jcol
        return remote(ref, dst.at[t], tsend.at[n], trecv.at[n, t], srow, scol)

    sends_tile = owner & jnp.logical_not(is_s | via_source)
    sends_u = sends_tile & jnp.logical_not(is_source)
    pl.when(is_source)(lambda: relay_in().start())
    for k in range(1, N_ROW):
        child_copy(k).start()
    pl.when(sends_tile)(lambda: v_copy().start())
    pl.when(sends_u)(lambda: u_copy().start())

    @pl.when(via_source)
    def _():
        via_in(0, vs).start()
        via_in(1, us).start()

    @pl.when(lends_out)
    def _():
        lend_copy(0, vs, vjoin).start()
        lend_copy(1, us, ujoin).start()

    loads[8].wait()
    for n in range(0, BB * BLK, 2 * BLK):
        back[n:n + 2 * BLK] = lax.dot_general(
            bt_v[:, n:n + 2 * BLK], ci_v[...], (((0,), (0,)), ((), ())),
            preferred_element_type=F32,
        ).astype(BF16)

    with jax.named_scope("child_wait"):
        all_children().wait_recv()
        total = childp[row]
        for k in range(N_ROW - 1):
            total = total + childrx[k]
        rowmsg[...] = total

    @pl.when(is_via)
    def _():
        via_in(0, vs).wait_recv()
        via_out(0, vs, vrx).start()
        via_in(1, us).wait_recv()
        via_out(1, us, urx).start()

    tiles = [(i, j) for i in range(G) for j in range(i)]

    def turn():
        with jax.named_scope("turn"):
            for jj in range(G):
                dt[jj] = d_v[jj].T
            for i, j in tiles:
                t = pair(i, j)
                utin[t] = urx[t].T.astype(BF16)
                wb[t] = nn(vrx[t].T.astype(BF16), dt[j]).astype(BF16)

    loads[7].wait()

    @pl.when(is_s)
    def _():
        with jax.named_scope("tiles_wait"):
            for i, j in ((3, 1), (3, 0), (3, 2), (1, 0), (2, 0), (2, 1)):
                t = pair(i, j)

                @pl.when(own_tile != t)
                def _():
                    with jax.named_scope(f"tv{i}{j}"):
                        remote(vs, vrx.at[t], tsend.at[0], trecv.at[0, t], srow, scol).wait_recv()
                    with jax.named_scope(f"tu{i}{j}"):
                        remote(us, urx.at[t], tsend.at[1], trecv.at[1, t], srow, scol).wait_recv()

                vbf[t] = vrx[t].astype(BF16)
                wf[t] = nn(urx[t].astype(BF16), d_v[i]).astype(BF16)
        pl.when(a == NG - 1)(turn)

    def is_older(b):
        return half + 2 * b + 1 < a

    with jax.named_scope("turn2"):
        for b in range(2):
            @pl.when(is_older(b))
            def _():
                ut[b] = u_v[b].T
                vt[b] = v_v[b].T

        @pl.when(is_join)
        def _():
            for jj in range(G):
                @pl.when(G * near + jj != JOIN)
                def _():
                    remote(
                        vs, vjoin.at[jj], tsend.at[0], jtile.at[0, jj], row, jnp.int32(0)
                    ).wait_recv()
                    remote(
                        us, ujoin.at[jj], tsend.at[1], jtile.at[1, jj], row, jnp.int32(0)
                    ).wait_recv()

                vj[jj] = vjoin[jj].astype(BF16)
                uj[jj] = ujoin[jj].astype(BF16)
                vjt[jj] = vjoin[jj].T.astype(BF16)
                ujt[jj] = ujoin[jj].T.astype(BF16)

    with jax.named_scope("fwd_row"):
        for b in range(2):
            @pl.when(is_older(b))
            def _():
                remote(xs.at[0], xrx.at[b], xsend.at[0], xrecv.at[b], srow, scol).wait_recv()
                p = nn(xrx[b].astype(BF16), v_v[b])
                p = jnp.where(live[b], p, 0.0).astype(BF16)
                rowmsg[...] += nn(p, u_v[b])

        @pl.when(is_join)
        def _():
            for jj in range(G):
                remote(
                    xs.at[0], xjoin.at[jj], xsend.at[0], xjrecv.at[jj], srow, scol
                ).wait_recv()
                p = nn(xjoin[jj].astype(BF16), vj[jj]).astype(BF16)
                rowmsg[...] += nn(p, uj[jj])

    def row_copy():
        return remote(
            rowmsg, srx.at[ii, col], msend.at[0], srecv.at[ii], srow, scol
        )

    @pl.when(is_s)
    def _():
        srx[ii, col] = rowmsg[...]

    @pl.when(jnp.logical_not(is_s))
    def _():
        row_copy().start()

    @pl.when(is_relay)
    def _():
        relay_in().wait_recv()
        relay_out().start()

    loads[6].wait()

    def x_copy(jj, da, i2):
        if da == 1:
            return remote(
                xs.at[jj], xjoin.at[jj], xsend.at[0], xjrecv.at[jj],
                G * (a + 1) + i2, jnp.int32(JOIN),
            )
        return remote(
            xs.at[jj], xrx.at[slot], xsend.at[da - 1], xrecv.at[slot],
            G * (a + da) + i2, ours + jj,
        )

    @pl.when(is_s)
    def _():
        def wait_row(jj, count):
            slots = srx.at[jj, pl.ds(0, count)]
            remote(slots, slots, msend.at[0], srecv.at[jj], srow, scol).wait_recv()

        def wait_all(jj):
            with jax.named_scope(f"s_fwd_wait{jj}"):
                pl.when(srel != jj)(lambda: wait_row(jj, N_COL))
                pl.when(srel == jj)(lambda: wait_row(jj, N_COL - 1))

        def base(jj):
            parts = [srx[jj, c] for c in range(N_COL)]
            while len(parts) > 1:
                parts = [parts[n] + parts[n + 1] for n in range(0, len(parts), 2)]
            right = rhs_v[:, jj * TILE:(jj + 1) * TILE].astype(F32) - parts[0]
            return folded(nn(two_halves(right), d_v[jj]))

        x = [None] * G

        send_rows = [pick(rows, a) for rows in SEND_ROWS]

        def publish(jj):
            xs[jj] = x[jj]

            @pl.when(a + 1 < NG)
            def _():
                for rank, j2 in SEND_ORDER[jj]:
                    x_copy(j2, 1, send_rows[rank]).start()

        wait_all(0)
        x[0] = base(0)
        publish(0)
        for jj in range(1, G):
            wait_all(jj)
            done = x[jj - 1].astype(BF16)
            for mm in range(jj, G):
                t = pair(mm, jj - 1)
                part = nn(nn(done, vbf[t]).astype(BF16), wf[t])
                x[mm] = part if x[mm] is None else x[mm] + part
            x[jj] = base(jj) - x[jj]
            publish(jj)
        for da in range(2, NG):
            @pl.when(a + da < NG)
            def _():
                for i2 in range(G):
                    for jj in range(G):
                        x_copy(jj, da, i2).start()
        pl.when(a < NG - 1)(turn)

    all_children().wait_send()
    @pl.when(via_source)
    def _():
        via_in(0, vs).wait_send()
        via_in(1, us).wait_send()

    @pl.when(is_via)
    def _():
        via_out(0, vs, vrx).wait_send()
        via_out(1, us, urx).wait_send()

    @pl.when(lends_out)
    def _():
        lend_copy(0, vs, vjoin).wait_send()
        lend_copy(1, us, ujoin).wait_send()

    pl.when(sends_tile)(lambda: v_copy().wait_send())
    pl.when(sends_u)(lambda: u_copy().wait_send())
    pl.when(is_source)(lambda: relay_in().wait_send())
    pl.when(is_relay)(lambda: relay_out().wait_send())
    pl.when(jnp.logical_not(is_s))(lambda: row_copy().wait_send())

    def z_tile(i):
        return zfull.at[pl.ds(QB * i, QB)]

    def z_copy(jj, k):
        c = mod(JOIN + k, N_COL)
        return c, remote(
            zs.at[jj], z_tile(G * a + jj), zsend.at[jj], zrecv.at[0], G * a + jj, c
        )

    may_be_own = {(SOLVER_COL[g] - JOIN) % N_COL for g in range(NG)}

    @pl.when(is_s)
    def _():
        def wait_da(jj, da):
            slots = brx.at[jj, pl.ds((da - 1) * G, G)]
            remote(slots, slots, bsend.at[0], brecv.at[jj, da - 1], srow, scol).wait_recv()

        def take(jj, da):
            n = (da - 1) * G
            tacc[jj] -= (brx[jj, n] + brx[jj, n + 1]) + (brx[jj, n + 2] + brx[jj, n + 3])

        def collect(rows, das):
            for da in das:
                @pl.when(a + da < NG)
                def _():
                    for jj in rows:
                        wait_da(jj, da)
                    for jj in rows:
                        take(jj, da)

        def base(jj):
            return folded(nn(two_halves(tacc[jj]), dt[jj]))

        z = [None] * G

        def publish(jj):
            for q in range(QB):
                part = z[jj][:, q * BLK:(q + 1) * BLK]
                zs[jj, q] = part
                zfull[QB * (G * a + jj) + q] = part
            for k in range(N_COL):
                c, copy = z_copy(jj, k)
                if k in may_be_own:
                    pl.when((srel != jj) | (c != col))(copy.start)
                else:
                    copy.start()

        tacc[...] = xs[...]
        with jax.named_scope("s_bwd_old"):
            collect(range(G), range(NG - 1, 1, -1))
        last = G - 1
        with jax.named_scope("s_bwd_wait3"):
            collect((last,), (1,))
        z[last] = base(last)
        publish(last)
        for jj in range(last - 1, -1, -1):
            with jax.named_scope(f"s_bwd_wait{jj}"):
                collect((jj,), (1,))
            done = z[jj + 1].astype(BF16)
            for mm in range(jj, -1, -1):
                t = pair(jj + 1, mm)
                part = nn(nn(done, utin[t]).astype(BF16), wb[t])
                z[mm] = part if z[mm] is None else z[mm] + part
            z[jj] = base(jj) - z[jj]
            publish(jj)

    @pl.when(jnp.logical_not(is_s))
    def _():
        with jax.named_scope("z_wait"):
            remote(zs.at[0], z_tile(row), zsend.at[0], zrecv.at[0], srow, scol).wait_recv()

    def back_copy(b):
        g = half + 2 * b
        n = (a - g - 1) * G + ii
        return remote(
            bmsg.at[b], brx.at[jcol, n], bsend.at[b], brecv.at[jcol, a - g - 1], *solver_of(g)
        )

    def join_copy(jj):
        return remote(
            bjoin.at[jj], brx.at[jj, ii], bjsend.at[0], brecv.at[jj, 0], *solver_of(a - 1)
        )

    @pl.when(is_join)
    def _():
        zb = jnp.concatenate([zfull[QB * row + q] for q in range(QB)], axis=1).astype(BF16)
        for jj in reversed(range(G)):
            bjoin[jj] = nn(nn(zb, ujt[jj]).astype(BF16), vjt[jj])
            join_copy(jj).start()

    mine = jnp.concatenate([zfull[QB * row + q] for q in range(QB)], axis=1)
    for b in reversed(range(2)):
        @pl.when(is_older(b))
        def _():
            q = nn(mine.astype(BF16), ut[b])
            q = jnp.where(live[b], q, 0.0).astype(BF16)
            bmsg[b] = nn(q, vt[b])
            back_copy(b).start()

    def gather_copy(k):
        peer = peer_row(NEAR_FIRST, k)
        return remote(z_tile(row), z_tile(row), gsend.at[0], grecv.at[0], peer, col)

    def all_gathered():
        every = zfull.at[pl.ds(0, QB * (N_ROW - 1))]
        return remote(every, every, gsend.at[0], grecv.at[0], srow, scol)

    for k in range(1, N_ROW):
        gather_copy(k).start()

    wide = zfull[QB * row + div(col, 2)]
    root_out[...] = jnp.where(mod(col, 2) == 0, wide[:, :HALF], wide[:, HALF:])

    for b in range(2):
        @pl.when(is_older(b))
        def _():
            back_copy(b).wait_send()

    @pl.when(is_join)
    def _():
        remote(bjoin, bjoin, bjsend.at[0], brecv.at[0, 0], srow, scol).wait_send()

    @pl.when(is_s)
    def _():
        for da in range(1, NG):
            @pl.when(a + da < NG)
            def _():
                slots = brx.at[:, pl.ds(0, G)]
                remote(slots, slots, xsend.at[da - 1], xrecv.at[0], srow, scol).wait_send()
        for jj in range(G):
            def wait_z(count):
                slots = srx.at[jj, pl.ds(0, count)]
                remote(slots, slots, zsend.at[jj], zrecv.at[0], srow, scol).wait_send()

            pl.when(srel != jj)(lambda: wait_z(N_COL))
            pl.when(srel == jj)(lambda: wait_z(N_COL - 1))

    with jax.named_scope("gather_wait"):
        all_gathered().wait_recv()

    with jax.named_scope("final"):
        parts = [zfull[blocks_s[0, m]] for m in range(BB)]
        gathered = jnp.concatenate(parts, axis=1).astype(BF16)
        child_out[0] = cx_v[...].astype(F32) - nn(gathered, back[...])

    all_gathered().wait_send()


def per_device(
    root_rhs, diag_inv, tile_u, tile_v, tile_rank, child_x, border_t, child_inv, child_blocks
):
    vmem = pl.BlockSpec(memory_space=pltpu.VMEM)
    hbm = pl.BlockSpec(memory_space=pltpu.HBM)
    dma = pltpu.SemaphoreType.DMA
    pairs = G * (G - 1) // 2
    wide = (RHS, TILE)
    return pl.pallas_call(
        kernel,
        out_shape=(
            jax.ShapeDtypeStruct((RHS, HALF), F32),
            jax.ShapeDtypeStruct((1, RHS, TILE), F32),
        ),
        in_specs=[hbm] * 9,
        out_specs=(vmem, vmem),
        scratch_shapes=[
            pltpu.VMEM((RHS, G * TILE), BF16),
            pltpu.VMEM(wide, BF16),
            pltpu.SMEM((1, BB), jnp.int32),
            pltpu.SMEM((1, 2), jnp.int32),
            pltpu.VMEM((RMAX, TILE), F32),
            pltpu.VMEM((G, TILE, TILE), BF16),
            pltpu.VMEM((2, TILE, RMAX), BF16),
            pltpu.VMEM((2, RMAX, TILE), BF16),
            pltpu.VMEM((pairs, TILE, RMAX), BF16),
            pltpu.VMEM((G, TILE, RMAX), F32),
            pltpu.VMEM((G, RMAX, TILE), F32),
            pltpu.VMEM((G, TILE, RMAX), BF16),
            pltpu.VMEM((G, RMAX, TILE), BF16),
            pltpu.VMEM((G, RMAX, TILE), BF16),
            pltpu.VMEM((G, TILE, RMAX), BF16),
            pltpu.VMEM((G, *wide), F32),
            pltpu.VMEM((G, *wide), F32),
            pltpu.VMEM((TILE, BB * BLK), BF16),
            pltpu.VMEM((TILE, TILE), BF16),
            pltpu.VMEM((2, RMAX, TILE), BF16),
            pltpu.VMEM((2, TILE, RMAX), BF16),
            pltpu.VMEM((G, TILE, TILE), BF16),
            pltpu.VMEM((RMAX, TILE), F32),
            pltpu.VMEM((TILE, RMAX), F32),
            pltpu.VMEM((pairs, RMAX, TILE), F32),
            pltpu.VMEM((pairs, TILE, RMAX), F32),
            pltpu.VMEM((pairs, RMAX, TILE), BF16),
            pltpu.VMEM((pairs, RMAX, TILE), BF16),
            pltpu.VMEM((pairs, TILE, RMAX), BF16),
            pltpu.VMEM((NT, *wide), F32),
            pltpu.VMEM((N_ROW, *wide), F32),
            pltpu.VMEM((2, *wide), F32),
            pltpu.VMEM(wide, F32),
            pltpu.VMEM((G, N_COL, *wide), F32),
            pltpu.VMEM((G, *wide), F32),
            pltpu.VMEM((NT * QB, RHS, BLK), F32),
            pltpu.VMEM((G, QB, RHS, BLK), F32),
            pltpu.VMEM((2, *wide), F32),
            pltpu.VMEM((G, (NG - 1) * G, *wide), F32),
            pltpu.VMEM((G, *wide), F32),
            dma((9,)),
            dma((1,)),
            dma((1,)),
            dma((2,)),
            dma((2, pairs)),
            dma((1,)),
            dma((G,)),
            dma((NG - 1,)),
            dma((2,)),
            dma((G,)),
            dma((1,)),
            dma((2,)),
            dma((G, NG - 1)),
            dma((1,)),
            dma((1,)),
            dma((1,)),
            dma((1,)),
            dma((2, G)),
            dma((G,)),
            dma((1,)),
            dma((2,)),
            pltpu.VMEM((BB * BLK, TILE), BF16),
        ],
        compiler_params=pltpu.CompilerParams(
            collective_id=0, has_side_effects=True, vmem_limit_bytes=48_000_000
        ),
    )(
        *(
            pltpu.with_memory_space_constraint(array, pltpu.HBM)
            for array in (
                root_rhs, child_x, child_blocks, tile_rank, diag_inv,
                tile_u, tile_v, border_t, child_inv,
            )
        )
    )


def solution(mesh):
    both = ("row", "col")
    tiles = P("row", "col", None, None, None, None)
    in_specs = (
        P(),
        P(),
        tiles,
        tiles,
        P("row", "col", None, None),
        P(both, None, None),
        P(both, None, None),
        P(both, None, None),
        P(both, None),
    )
    out_specs = (P(None, both), P(both, None, None))
    return jax.shard_map(
        per_device, mesh=mesh, in_specs=in_specs, out_specs=out_specs, check_vma=False
    )
```
